16 devices in a mesh: dp: 2 (over y, z), sp: 8 (over x, core).
Axes of the slice: x: 4, y: 2, z: 1, core: 2. Of those that a mesh axis runs over, the one named last changes fastest.
The devices are a block of a 4x4x8 slice.
Arguments:
- hidden: bfloat16 [49152, 2048], P(('dp', 'sp')), parts along dimension 0
- tok_perm: int32 [49152], P(('dp', 'sp')), parts along dimension 0
- send_off: int32 [128], P(('dp', 'sp')), parts along dimension 0
- send_len: int32 [128], P(('dp', 'sp')), parts along dimension 0
- recv_off: int32 [128], P(('dp', 'sp')), parts along dimension 0
- recv_len: int32 [128], P(('dp', 'sp')), parts along dimension 0
- recv_doc: int32 [24576], P(('dp', 'sp')), parts along dimension 0
- recv_pos: int32 [24576], P(('dp', 'sp')), parts along dimension 0
- g_attn: bfloat16 [2048], replicated
- w_q: bfloat16 [2048, 32, 64], replicated
- w_k: bfloat16 [2048, 32, 64], replicated
- w_v: bfloat16 [2048, 32, 64], replicated
- w_o: bfloat16 [32, 64, 2048], replicated
- g_mlp: bfloat16 [2048], replicated
- w_gate: bfloat16 [2048, 8192], replicated
- w_up: bfloat16 [2048, 8192], replicated
- w_down: bfloat16 [8192, 2048], replicated
Outputs:
- output: bfloat16 [49152, 2048], P(('dp', 'sp')), parts along dimension 0
There are 2 independent parts. The reference program is written for one: setup_inputs(seed, part) draws one part's arguments, and reference() takes and returns one part's arrays. A program takes and returns all parts, laid end to end along the dimension named above; an argument that names none is the same for every part.
All inputs are finite; a program needn't handle non-finite values.
Results may differ from the reference program's by a relative error of at most 0.0121102.
Values are sent between devices in bfloat16 or wider.
A program may use at most 768 MiB of HBM per device.

```python
import jax
import jax.numpy as jnp
from jax import lax

GROUP_SIZE = 8
TOKENS_DEV = 3072
D = 2048
HEADS = 32
KV_HEADS = 32
HEAD = 64
FF = 8192
PIECES = 4
Q_BLOCK = 128
ROPE_BASE = 500000
RECV_CAP = TOKENS_DEV // 2
Q_PER_KV = HEADS // KV_HEADS
NORM_EPS = 1e-5


def draw_plan(plan_key):
    key_src, key_shift, key_long = jax.random.split(plan_key, 3)
    src_of = jax.vmap(lambda sub_key: jax.random.permutation(sub_key, GROUP_SIZE))(jax.random.split(key_src, PIECES)).astype(jnp.int32)
    dev_ids = jnp.arange(GROUP_SIZE, dtype=jnp.int32)
    len_shift = jax.random.randint(key_shift, (GROUP_SIZE,), 0, 6, dtype=jnp.int32)
    long_dev = jax.random.randint(key_long, (), 0, GROUP_SIZE, dtype=jnp.int32)
    len_shift = jnp.where(dev_ids == long_dev, 0, len_shift).astype(jnp.int32)
    first_len = jnp.right_shift(jnp.full((GROUP_SIZE,), RECV_CAP, jnp.int32), len_shift)
    rest_len = RECV_CAP - first_len
    piece_len = jnp.stack([first_len, rest_len // 3, (rest_len + 1) // 3, (rest_len + 2) // 3]).astype(jnp.int32)
    held_dest = jnp.argsort(src_of, axis=1).astype(jnp.int32)
    held_len = jnp.take_along_axis(piece_len, held_dest, axis=1)
    held_end = jnp.cumsum(held_len, axis=0)
    tok_idx = jnp.arange(TOKENS_DEV, dtype=jnp.int32)
    piece_idx = jnp.sum((tok_idx[None, None, :] >= held_end[:, :, None]).astype(jnp.int32), axis=0)
    dest_pad = jnp.concatenate([held_dest, jnp.full((1, GROUP_SIZE), GROUP_SIZE, jnp.int32)], axis=0)
    tok_dest = jnp.take_along_axis(dest_pad.T, piece_idx, axis=1)
    tok_perm = jnp.argsort(tok_dest * TOKENS_DEV + tok_idx[None, :], axis=1)
    to_dest = (held_dest[:, :, None] == dev_ids[None, None, :]).astype(jnp.int32)
    send_len = jnp.sum(to_dest * held_len[:, :, None], axis=0)
    send_off = jnp.cumsum(send_len, axis=1) - send_len
    recv_len = send_len.T
    recv_off = jnp.cumsum(recv_len, axis=1) - recv_len
    order_key = src_of * PIECES + jnp.arange(PIECES, dtype=jnp.int32)[:, None]
    earlier = (order_key[None, :, :] < order_key[:, None, :]).astype(jnp.int32)
    dest_start = jnp.sum(earlier * piece_len[None, :, :], axis=1)
    slot_idx = jnp.arange(RECV_CAP, dtype=jnp.int32)
    in_piece = ((slot_idx[None, None, :] >= dest_start[:, :, None]) & (slot_idx[None, None, :] < (dest_start + piece_len)[:, :, None])).astype(jnp.int32)
    recv_doc = jnp.sum(in_piece * order_key[:, :, None], axis=0)
    recv_pos = jnp.sum(in_piece * (slot_idx[None, None, :] - dest_start[:, :, None]), axis=0)
    return {
        "tok_perm": tok_perm.reshape(-1).astype(jnp.int32),
        "send_off": send_off.reshape(-1).astype(jnp.int32),
        "send_len": send_len.reshape(-1).astype(jnp.int32),
        "recv_off": recv_off.reshape(-1).astype(jnp.int32),
        "recv_len": recv_len.reshape(-1).astype(jnp.int32),
        "recv_doc": recv_doc.reshape(-1).astype(jnp.int32),
        "recv_pos": recv_pos.reshape(-1).astype(jnp.int32),
    }


def setup_inputs(seed: int = 0, part: int = 0) -> dict:
    base_key = jax.random.key(seed)
    part_key = jax.random.fold_in(base_key, part)
    key_hidden, key_plan = jax.random.split(part_key)
    weight_keys = jax.random.split(base_key, 9)
    plan_ints = draw_plan(key_plan)
    qk_std = 1.7 * D ** -0.5

    def normal_w(index, shape, std):
        return (jax.random.normal(weight_keys[index], shape, jnp.float32) * std).astype(jnp.bfloat16)

    def draw_gain(index):
        return jax.random.uniform(weight_keys[index], (D,), jnp.float32, 0.5, 1.5).astype(jnp.bfloat16)

    return {
        "hidden": jax.random.normal(key_hidden, (GROUP_SIZE * TOKENS_DEV, D), jnp.float32).astype(jnp.bfloat16),
        "tok_perm": plan_ints["tok_perm"],
        "send_off": plan_ints["send_off"],
        "send_len": plan_ints["send_len"],
        "recv_off": plan_ints["recv_off"],
        "recv_len": plan_ints["recv_len"],
        "recv_doc": plan_ints["recv_doc"],
        "recv_pos": plan_ints["recv_pos"],
        "g_attn": draw_gain(0),
        "w_q": normal_w(1, (D, HEADS, HEAD), qk_std),
        "w_k": normal_w(2, (D, KV_HEADS, HEAD), qk_std),
        "w_v": normal_w(3, (D, KV_HEADS, HEAD), D ** -0.5),
        "w_o": normal_w(4, (HEADS, HEAD, D), (HEADS * HEAD) ** -0.5),
        "g_mlp": draw_gain(5),
        "w_gate": normal_w(6, (D, FF), D ** -0.5),
        "w_up": normal_w(7, (D, FF), D ** -0.5),
        "w_down": normal_w(8, (FF, D), FF ** -0.5),
    }


def rms_norm(rows_in, gain_vec):
    rows_f = rows_in.astype(jnp.float32)
    inv_rms = lax.rsqrt(jnp.mean(rows_f * rows_f, axis=-1, keepdims=True) + NORM_EPS)
    return (rows_f * inv_rms * gain_vec.astype(jnp.float32)).astype(jnp.bfloat16)


def rope(proj, positions):
    half_dim = HEAD // 2
    inv_freq = jnp.power(jnp.float32(ROPE_BASE), -2.0 * jnp.arange(half_dim, dtype=jnp.float32) / HEAD)
    angles = positions.astype(jnp.float32)[:, None, None] * inv_freq[None, None, :]
    cos_t = jnp.cos(angles)
    sin_t = jnp.sin(angles)
    lo_half = proj[..., :half_dim]
    hi_half = proj[..., half_dim:]
    return jnp.concatenate([lo_half * cos_t - hi_half * sin_t, hi_half * cos_t + lo_half * sin_t], axis=-1)


def attend(q_rot, k_rot, v_proj, doc_ids, positions):
    k_f = k_rot.astype(jnp.float32)
    v_f = v_proj.astype(jnp.float32)
    n_blocks = RECV_CAP // Q_BLOCK

    def one_block(blk_args):
        q_blk, doc_q, pos_q = blk_args
        scores = jnp.einsum("qkgd,skd->kgqs", q_blk.astype(jnp.float32), k_f) * (HEAD ** -0.5)
        allowed = (doc_q[:, None] == doc_ids[None, :]) & (positions[None, :] <= pos_q[:, None])
        probs_bf = jax.nn.softmax(jnp.where(allowed, scores, -1e30), axis=-1).astype(jnp.bfloat16)
        return jnp.einsum("kgqs,skd->qkgd", probs_bf.astype(jnp.float32), v_f).astype(jnp.bfloat16)

    blocks_out = lax.map(one_block, (q_rot.reshape(n_blocks, Q_BLOCK, KV_HEADS, Q_PER_KV, HEAD), doc_ids.reshape(n_blocks, Q_BLOCK), positions.reshape(n_blocks, Q_BLOCK)))
    return blocks_out.reshape(RECV_CAP, HEADS * HEAD)


def layer(dest_rows, doc_ids, positions, g_attn, w_q, w_k, w_v, w_o, g_mlp, w_gate, w_up, w_down):
    normed = rms_norm(dest_rows, g_attn)
    q_proj = jnp.dot(normed, w_q.reshape(D, HEADS * HEAD), preferred_element_type=jnp.float32).reshape(RECV_CAP, HEADS, HEAD)
    k_proj = jnp.dot(normed, w_k.reshape(D, KV_HEADS * HEAD), preferred_element_type=jnp.float32).reshape(RECV_CAP, KV_HEADS, HEAD)
    v_proj = jnp.dot(normed, w_v.reshape(D, KV_HEADS * HEAD), preferred_element_type=jnp.float32).astype(jnp.bfloat16).reshape(RECV_CAP, KV_HEADS, HEAD)
    q_rot = rope(q_proj, positions).astype(jnp.bfloat16).reshape(RECV_CAP, KV_HEADS, Q_PER_KV, HEAD)
    k_rot = rope(k_proj, positions).astype(jnp.bfloat16)
    attn_heads = attend(q_rot, k_rot, v_proj, doc_ids, positions)
    attn_out = jnp.dot(attn_heads, w_o.reshape(HEADS * HEAD, D), preferred_element_type=jnp.float32).astype(jnp.bfloat16)
    resid_mid = (dest_rows.astype(jnp.float32) + attn_out.astype(jnp.float32)).astype(jnp.bfloat16)
    normed_mlp = rms_norm(resid_mid, g_mlp)
    gate_proj = jnp.dot(normed_mlp, w_gate, preferred_element_type=jnp.float32)
    up_proj = jnp.dot(normed_mlp, w_up, preferred_element_type=jnp.float32)
    hidden_act = (jax.nn.silu(gate_proj) * up_proj).astype(jnp.bfloat16)
    down_proj = jnp.dot(hidden_act, w_down, preferred_element_type=jnp.float32).astype(jnp.bfloat16)
    return (resid_mid.astype(jnp.float32) + down_proj.astype(jnp.float32)).astype(jnp.bfloat16)


def reference(hidden, tok_perm, send_off, send_len, recv_off, recv_len, recv_doc, recv_pos, g_attn, w_q, w_k, w_v, w_o, g_mlp, w_gate, w_up, w_down):
    perm_rows = tok_perm.reshape(GROUP_SIZE, TOKENS_DEV)
    send_off_m = send_off.reshape(GROUP_SIZE, GROUP_SIZE)
    send_len_m = send_len.reshape(GROUP_SIZE, GROUP_SIZE)
    recv_off_m = recv_off.reshape(GROUP_SIZE, GROUP_SIZE)
    recv_len_m = recv_len.reshape(GROUP_SIZE, GROUP_SIZE)
    doc_rows = recv_doc.reshape(GROUP_SIZE, RECV_CAP)
    pos_rows = recv_pos.reshape(GROUP_SIZE, RECV_CAP)
    dev_ids = jnp.arange(GROUP_SIZE)
    slot_idx = jnp.arange(RECV_CAP)
    sorted_idx = jnp.arange(TOKENS_DEV)

    def one_dest(dest_dev):
        run_start = recv_off_m[dest_dev]
        in_run = (slot_idx[:, None] >= run_start[None, :]) & (slot_idx[:, None] < (run_start + recv_len_m[dest_dev])[None, :])
        src_dev = jnp.clip(jnp.sum(jnp.where(in_run, dev_ids[None, :], 0), axis=1), 0, GROUP_SIZE - 1)
        src_pos = jnp.sum(jnp.where(in_run, send_off_m[:, dest_dev][None, :] + slot_idx[:, None] - run_start[None, :], 0), axis=1)
        src_pos = jnp.clip(src_pos, 0, TOKENS_DEV - 1)
        filled = jnp.any(in_run, axis=1)
        src_row = src_dev * TOKENS_DEV + perm_rows[src_dev, src_pos]
        dest_rows = jnp.where(filled[:, None], hidden[src_row], jnp.zeros((), jnp.bfloat16))
        return layer(dest_rows, doc_rows[dest_dev], pos_rows[dest_dev], g_attn, w_q, w_k, w_v, w_o, g_mlp, w_gate, w_up, w_down)

    layer_rows = lax.map(one_dest, dev_ids).reshape(GROUP_SIZE * RECV_CAP, D)

    def one_source(src_dev):
        run_start = send_off_m[src_dev]
        in_run = (sorted_idx[:, None] >= run_start[None, :]) & (sorted_idx[:, None] < (run_start + send_len_m[src_dev])[None, :])
        dest_dev = jnp.clip(jnp.sum(jnp.where(in_run, dev_ids[None, :], 0), axis=1), 0, GROUP_SIZE - 1)
        dest_slot = jnp.sum(jnp.where(in_run, recv_off_m[:, src_dev][None, :] + sorted_idx[:, None] - run_start[None, :], 0), axis=1)
        dest_slot = jnp.clip(dest_slot, 0, RECV_CAP - 1)
        was_sent = jnp.any(in_run, axis=1)
        back_rows = jnp.where(was_sent[:, None], layer_rows[dest_dev * RECV_CAP + dest_slot], jnp.zeros((), jnp.bfloat16))
        inv_perm = jnp.argsort(perm_rows[src_dev])
        return back_rows[inv_perm]

    return lax.map(one_source, dev_ids).reshape(GROUP_SIZE * TOKENS_DEV, D)
```

```python
import functools

import jax
import jax.numpy as jnp
import numpy as np
from jax import lax
from jax.experimental import pallas as pl
from jax.experimental.pallas import tpu as pltpu
from jax.sharding import PartitionSpec as P

ROPE_BASE = 500000.0
NORM_EPS = 1e-5
Q_TILE = 256
QKV_TILE = 512


def rms_norm(rows_in, gain_vec):
    rows_f = rows_in.astype(jnp.float32)
    inv_rms = lax.rsqrt(jnp.mean(rows_f * rows_f, axis=-1, keepdims=True) + NORM_EPS)
    return (rows_f * inv_rms * gain_vec.astype(jnp.float32)).astype(jnp.bfloat16)


def rope_tables(positions, head_dim):
    half = head_dim // 2
    inv_freq = jnp.power(jnp.float32(ROPE_BASE), -2.0 * jnp.arange(half, dtype=jnp.float32) / head_dim)
    angles = positions.astype(jnp.float32)[:, None] * inv_freq[None, :]
    cos_t = jnp.cos(angles)
    sin_t = jnp.sin(angles)
    return jnp.concatenate([cos_t] * 4, axis=1), jnp.concatenate([-sin_t, sin_t] * 2, axis=1)


def qkv_proj(normed, w_q, w_k, w_v, cos_t, sin_t):
    rows, model_dim = normed.shape
    n_heads, head_dim = w_q.shape[1:]
    width = n_heads * head_dim
    w_all = [w.transpose(1, 2, 0).reshape(width, model_dim) for w in (w_q, w_k, w_v)]
    outs = []
    for kind, w in enumerate(w_all):
        outs.append(pl.pallas_call(
            functools.partial(qkv_one, head_dim, kind),
            out_shape=jax.ShapeDtypeStruct((rows, width), jnp.bfloat16),
            grid=(width // QKV_TILE,),
            in_specs=[
                pl.BlockSpec((rows, model_dim), lambda n: (0, 0)),
                pl.BlockSpec((QKV_TILE, model_dim), lambda n: (n, 0)),
                pl.BlockSpec(cos_t.shape, lambda n: (0, 0)),
                pl.BlockSpec(sin_t.shape, lambda n: (0, 0)),
            ],
            out_specs=pl.BlockSpec((rows, QKV_TILE), lambda n: (0, n)),
            compiler_params=pltpu.CompilerParams(vmem_limit_bytes=48 * 1024 * 1024),
            cost_estimate=pl.CostEstimate(flops=2 * rows * model_dim * width, bytes_accessed=2 * (2 * rows * model_dim + model_dim * width), transcendentals=0),
            name="qkv",
        )(normed, w, cos_t, sin_t))
    return outs


def qkv_one(head_dim, kind, h_ref, w_ref, cos_ref, sin_ref, o_ref):
    rows, cols = o_ref.shape
    lanes = cos_ref.shape[1]
    half = head_dim // 2
    step = 256
    scale = head_dim ** -0.5 if kind == 0 else 1.0

    @pl.loop(0, rows // step)
    def _(t):
        at = pl.ds(pl.multiple_of(t * step, step), step)
        acc = lax.dot_general(h_ref[at, :], w_ref[...], (((1,), (1,)), ((), ())), preferred_element_type=jnp.float32)
        if kind == 2:
            o_ref[at, :] = acc.astype(o_ref.dtype)
        else:
            cos_t = cos_ref[at, :]
            sin_t = sin_ref[at, :]
            first = lax.rem(lax.broadcasted_iota(jnp.int32, cos_t.shape, 1), head_dim) < half
            for b in range(cols // lanes):
                x = acc[:, b * lanes:(b + 1) * lanes]
                swapped = jnp.where(first, pltpu.roll(x, lanes - half, 1), pltpu.roll(x, half, 1))
                rot = (x * cos_t + swapped * sin_t) * scale
                o_ref[at, b * lanes:(b + 1) * lanes] = rot.astype(o_ref.dtype)


def attn_kernel(head_dim, q_ref, k_ref, v_ref, meta_row_ref, meta_col_ref, o_ref, bias_ref):
    rows, lanes = q_ref.shape
    n_tiles = rows // Q_TILE

    @pl.when(pl.program_id(0) == 0)
    def _():
        for t in range(n_tiles):
            at = slice(t * Q_TILE, (t + 1) * Q_TILE)
            n_keys = (t + 1) * Q_TILE
            ok = (meta_col_ref[at, 0:1] == meta_row_ref[0:1, :n_keys]) & (meta_row_ref[1:2, :n_keys] <= meta_col_ref[at, 1:2])
            bias_ref[at, :n_keys] = jnp.where(ok, 0.0, -1e30).astype(jnp.float32)

    lane = lax.broadcasted_iota(jnp.int32, (Q_TILE, lanes), 1)
    for t in range(n_tiles):
        at = slice(t * Q_TILE, (t + 1) * Q_TILE)
        n_keys = (t + 1) * Q_TILE
        q_blk = q_ref[at, :]
        heads_out = []
        for h in range(lanes // head_dim):
            mine = (lane >= h * head_dim) & (lane < (h + 1) * head_dim)
            q_h = jnp.where(mine, q_blk, jnp.zeros((), q_blk.dtype))
            s = lax.dot_general(q_h, k_ref[:n_keys, :], (((1,), (1,)), ((), ())), preferred_element_type=jnp.float32)
            s = s + bias_ref[at, :n_keys]
            top = jnp.max(s, axis=1, keepdims=True)
            e = jnp.exp(s - top)
            total = jnp.sum(e, axis=1, keepdims=True)
            o_h = jnp.dot(e.astype(jnp.bfloat16), v_ref[:n_keys, :], preferred_element_type=jnp.float32)
            heads_out.append(jnp.where(mine, o_h / total, 0.0))
        o_ref[at, :] = sum(heads_out).astype(o_ref.dtype)


def attention(q, k, v, doc_ids, positions, head_dim):
    rows, width = q.shape
    lanes = 128
    meta = jnp.stack([doc_ids, positions])
    head_spec = pl.BlockSpec((rows, lanes), lambda n: (0, n))
    whole = lambda a: pl.BlockSpec(a.shape, lambda n: (0, 0))
    meta_t = meta.T
    return pl.pallas_call(
        functools.partial(attn_kernel, head_dim),
        out_shape=jax.ShapeDtypeStruct((rows, width), jnp.bfloat16),
        grid=(width // lanes,),
        in_specs=[head_spec, head_spec, head_spec, whole(meta), whole(meta_t)],
        out_specs=head_spec,
        scratch_shapes=[pltpu.VMEM((rows, rows), jnp.float32)],
        compiler_params=pltpu.CompilerParams(vmem_limit_bytes=56 * 1024 * 1024),
        cost_estimate=pl.CostEstimate(flops=3 * rows * rows * width, bytes_accessed=8 * rows * width, transcendentals=rows * rows * width // 128),
        name="attention",
    )(q, k, v, meta, meta_t)


def layer(dest_rows, doc_ids, positions, g_attn, w_q, w_k, w_v, w_o, g_mlp, w_gate, w_up, w_down):
    model_dim = dest_rows.shape[1]
    n_heads, head_dim = w_q.shape[1:]
    cos_t, sin_t = rope_tables(positions, head_dim)
    normed = rms_norm(dest_rows, g_attn)
    q, k, v = qkv_proj(normed, w_q, w_k, w_v, cos_t, sin_t)
    attn_heads = attention(q, k, v, doc_ids, positions, head_dim)
    attn_out = jnp.dot(attn_heads, w_o.reshape(n_heads * head_dim, model_dim), preferred_element_type=jnp.float32).astype(jnp.bfloat16)
    resid_mid = (dest_rows.astype(jnp.float32) + attn_out.astype(jnp.float32)).astype(jnp.bfloat16)
    normed_mlp = rms_norm(resid_mid, g_mlp)
    gate_proj = jnp.dot(normed_mlp, w_gate, preferred_element_type=jnp.float32)
    up_proj = jnp.dot(normed_mlp, w_up, preferred_element_type=jnp.float32)
    hidden_act = (jax.nn.silu(gate_proj) * up_proj).astype(jnp.bfloat16)
    down_proj = jnp.dot(hidden_act, w_down, preferred_element_type=jnp.float32).astype(jnp.bfloat16)
    return (resid_mid.astype(jnp.float32) + down_proj.astype(jnp.float32)).astype(jnp.bfloat16)


def relay_tables(group):
    n_relay = group
    relay_of = np.array([[c for c in range(n_relay)] for i in range(group)])
    source_of = np.array([[i for i in range(group)] for k in range(group)])
    residue = np.array([[int(np.where(relay_of[source_of[k, m]] == k)[0][0]) for m in range(n_relay)] for k in range(group)])
    return relay_of, source_of, residue


def ceil_div(a, b):
    return -((-a) // b)


def pick(table, index, n):
    return jnp.sum(jnp.where(index[:, None] == jnp.arange(n)[None, :], table[None, :], 0), axis=1)


def plan_indices(me, len_ij, tok_perm, n_tok, n_cap, cap1, cap2, relay_of, source_of, residue):
    group, n_relay = relay_of.shape
    off_ij = jnp.cumsum(len_ij, axis=1) - len_ij
    roff_ij = jnp.cumsum(len_ij, axis=0) - len_ij
    res = np.arange(n_relay)
    first = ceil_div(off_ij[:, None, :] - res[None, :, None], n_relay)
    count = ceil_div((off_ij + len_ij)[:, None, :] - res[None, :, None], n_relay) - first
    first_k = first[source_of, residue]
    count_k = count[source_of, residue]
    base_k = jnp.cumsum(count_k, axis=1) - count_k
    end_k = base_k + count_k

    def mine(t):
        return lax.dynamic_index_in_dim(t, me, 0, keepdims=False)

    base_me, end_me, first_me = mine(base_k), mine(end_k), mine(first_k)
    q = jnp.arange(cap2)
    in_m = (q[None, None, :] >= base_me[:, :, None]) & (q[None, None, :] < end_me[:, :, None])
    src = jnp.arange(n_relay)[:, None, None] * cap1 + first_me[:, :, None] + q[None, None, :] - base_me[:, :, None]
    relay_idx = jnp.sum(jnp.where(in_m, src, 0), axis=0).reshape(-1)

    slot = jnp.arange(cap1)
    in_j = (slot[None, None, :] >= first_me[:, :, None]) & (slot[None, None, :] < (first_me + end_me - base_me)[:, :, None])
    back = jnp.arange(group)[None, :, None] * cap2 + base_me[:, :, None] + slot[None, None, :] - first_me[:, :, None]
    relay_back_idx = jnp.sum(jnp.where(in_j, back, 0), axis=1).reshape(-1)

    len_me = lax.dynamic_index_in_dim(len_ij, me, 1, keepdims=False)
    off_me = lax.dynamic_index_in_dim(off_ij, me, 1, keepdims=False)
    roff_me = lax.dynamic_index_in_dim(roff_ij, me, 1, keepdims=False)
    base_ic = jnp.zeros((group, n_relay), jnp.int32)
    base_to_me = lax.dynamic_index_in_dim(base_k, me, 2, keepdims=False)
    first_to_me = lax.dynamic_index_in_dim(first, me, 2, keepdims=False)
    place = np.zeros((group, n_relay), np.int32)
    for k in range(group):
        for m in range(n_relay):
            place[source_of[k, m], residue[k, m]] = k * n_relay + m
    base_ic = base_to_me.reshape(-1)[place]
    table = relay_of * cap2 + base_ic - first_to_me
    u = jnp.arange(n_cap)
    in_i = (u[:, None] >= roff_me[None, :]) & (u[:, None] < (roff_me + len_me)[None, :])
    r_of_u = jnp.sum(jnp.where(in_i, off_me[None, :] + u[:, None] - roff_me[None, :], 0), axis=1)
    i_of_u = jnp.sum(jnp.where(in_i, np.arange(group)[None, :], 0), axis=1)
    c_of_u = lax.rem(r_of_u, n_relay)
    dest_idx = pick(table.reshape(-1), i_of_u * n_relay + c_of_u, group * n_relay) + r_of_u // n_relay

    count_to_me = lax.dynamic_index_in_dim(count_k, me, 2, keepdims=False)
    first_km = lax.dynamic_index_in_dim(first_k, me, 2, keepdims=False)
    in_km = (q[None, None, :] >= base_to_me[:, :, None]) & (q[None, None, :] < (base_to_me + count_to_me)[:, :, None])
    r_km = (first_km[:, :, None] + q[None, None, :] - base_to_me[:, :, None]) * n_relay + residue[:, :, None]
    u_km = r_km + (roff_me - off_me)[source_of][:, :, None]
    dest_back_idx = jnp.sum(jnp.where(in_km, u_km, 0), axis=1).reshape(-1)

    used = jnp.sum(lax.dynamic_index_in_dim(len_ij, me, 0, keepdims=False))
    r = jnp.arange(cap1)[None, :] * n_relay + res[:, None]
    send_idx = jnp.pad(tok_perm, (0, cap1 * n_relay - n_tok)).reshape(cap1, n_relay).T.reshape(-1)
    inv_perm = jnp.argsort(tok_perm)
    final_idx = lax.rem(inv_perm, n_relay) * cap1 + inv_perm // n_relay
    return send_idx, relay_idx, dest_idx, dest_back_idx, relay_back_idx, final_idx, inv_perm < used


def solution(mesh):
    row_spec = P(('dp', 'sp'), None)
    vec_spec = P(('dp', 'sp'))
    rep_spec = P()

    def per_device(hidden, tok_perm, send_off, send_len, recv_off, recv_len, recv_doc, recv_pos, g_attn, w_q, w_k, w_v, w_o, g_mlp, w_gate, w_up, w_down):
        n_tok, model_dim = hidden.shape
        n_cap = recv_doc.shape[0]
        group = send_off.shape[0]
        relay_of, source_of, residue = relay_tables(group)
        n_relay = relay_of.shape[1]
        cap1 = -(-n_tok // n_relay)
        cap2 = -(-(n_cap + n_relay * (n_relay - 1)) // n_relay)
        cap2 = -(-cap2 // 8) * 8
        me = lax.axis_index('sp')
        len_ij = lax.all_gather(send_len, 'sp')
        send_idx, relay_idx, dest_idx, dest_back_idx, relay_back_idx, final_idx, was_sent = plan_indices(
            me, len_ij, tok_perm, n_tok, n_cap, cap1, cap2, relay_of, source_of, residue)

        def take(rows, index):
            return rows.at[index].get(mode='promise_in_bounds')

        def exchange(rows, cap):
            return lax.all_to_all(rows.reshape(-1, cap, model_dim), 'sp', 0, 0, tiled=True).reshape(-1, model_dim)

        relay_rows = exchange(take(hidden, send_idx), cap1)
        dest_rows = take(exchange(take(relay_rows, relay_idx), cap2), dest_idx)
        out_rows = layer(dest_rows, recv_doc, recv_pos, g_attn, w_q, w_k, w_v, w_o, g_mlp, w_gate, w_up, w_down)
        relay_back = exchange(take(out_rows, dest_back_idx), cap2)
        src_back = exchange(take(relay_back, relay_back_idx), cap1)
        return jnp.where(was_sent[:, None], take(src_back, final_idx), jnp.zeros((), hidden.dtype))

    return jax.shard_map(per_device, mesh=mesh, in_specs=(row_spec,) + (vec_spec,) * 7 + (rep_spec,) * 9, out_specs=row_spec, check_vma=False)
```

```python
import functools

import jax
import jax.numpy as jnp
import numpy as np
from jax import lax
from jax.experimental import pallas as pl
from jax.experimental.pallas import tpu as pltpu
from jax.sharding import PartitionSpec as P

ROPE_BASE = 500000.0
NORM_EPS = 1e-5
Q_TILE = 256
QKV_TILE = 512


def rms_norm(rows_in, gain_vec):
    rows_f = rows_in.astype(jnp.float32)
    inv_rms = lax.rsqrt(jnp.mean(rows_f * rows_f, axis=-1, keepdims=True) + NORM_EPS)
    return (rows_f * inv_rms * gain_vec.astype(jnp.float32)).astype(jnp.bfloat16)


def rope_tables(positions, head_dim):
    half = head_dim // 2
    inv_freq = jnp.power(jnp.float32(ROPE_BASE), -2.0 * jnp.arange(half, dtype=jnp.float32) / head_dim)
    angles = positions.astype(jnp.float32)[:, None] * inv_freq[None, :]
    cos_t = jnp.cos(angles)
    sin_t = jnp.sin(angles)
    return jnp.concatenate([cos_t] * 4, axis=1), jnp.concatenate([-sin_t, sin_t] * 2, axis=1)


def qkv_proj(normed, w_q, w_k, w_v, cos_t, sin_t):
    rows, model_dim = normed.shape
    n_heads, head_dim = w_q.shape[1:]
    width = n_heads * head_dim
    w_all = [w.transpose(1, 2, 0).reshape(width, model_dim) for w in (w_q, w_k, w_v)]
    outs = []
    for kind, w in enumerate(w_all):
        outs.append(pl.pallas_call(
            functools.partial(qkv_one, head_dim, kind),
            out_shape=jax.ShapeDtypeStruct((rows, width), jnp.bfloat16),
            grid=(width // QKV_TILE,),
            in_specs=[
                pl.BlockSpec((rows, model_dim), lambda n: (0, 0)),
                pl.BlockSpec((QKV_TILE, model_dim), lambda n: (n, 0)),
                pl.BlockSpec(cos_t.shape, lambda n: (0, 0)),
                pl.BlockSpec(sin_t.shape, lambda n: (0, 0)),
            ],
            out_specs=pl.BlockSpec((rows, QKV_TILE), lambda n: (0, n)),
            compiler_params=pltpu.CompilerParams(vmem_limit_bytes=48 * 1024 * 1024),
            cost_estimate=pl.CostEstimate(flops=2 * rows * model_dim * width, bytes_accessed=2 * (2 * rows * model_dim + model_dim * width), transcendentals=0),
            name="qkv",
        )(normed, w, cos_t, sin_t))
    return outs


def qkv_one(head_dim, kind, h_ref, w_ref, cos_ref, sin_ref, o_ref):
    rows, cols = o_ref.shape
    lanes = cos_ref.shape[1]
    half = head_dim // 2
    step = 256
    scale = head_dim ** -0.5 if kind == 0 else 1.0

    @pl.loop(0, rows // step)
    def _(t):
        at = pl.ds(pl.multiple_of(t * step, step), step)
        acc = lax.dot_general(h_ref[at, :], w_ref[...], (((1,), (1,)), ((), ())), preferred_element_type=jnp.float32)
        if kind == 2:
            o_ref[at, :] = acc.astype(o_ref.dtype)
        else:
            cos_t = cos_ref[at, :]
            sin_t = sin_ref[at, :]
            first = lax.rem(lax.broadcasted_iota(jnp.int32, cos_t.shape, 1), head_dim) < half
            for b in range(cols // lanes):
                x = acc[:, b * lanes:(b + 1) * lanes]
                swapped = jnp.where(first, pltpu.roll(x, lanes - half, 1), pltpu.roll(x, half, 1))
                rot = (x * cos_t + swapped * sin_t) * scale
                o_ref[at, b * lanes:(b + 1) * lanes] = rot.astype(o_ref.dtype)


def attn_kernel(head_dim, q_ref, k_ref, v_ref, meta_row_ref, meta_col_ref, o_ref, bias_ref):
    rows, lanes = q_ref.shape
    n_tiles = rows // Q_TILE

    @pl.when(pl.program_id(0) == 0)
    def _():
        for t in range(n_tiles):
            at = slice(t * Q_TILE, (t + 1) * Q_TILE)
            n_keys = (t + 1) * Q_TILE
            ok = (meta_col_ref[at, 0:1] == meta_row_ref[0:1, :n_keys]) & (meta_row_ref[1:2, :n_keys] <= meta_col_ref[at, 1:2])
            bias_ref[at, :n_keys] = jnp.where(ok, 0.0, -1e30).astype(jnp.float32)

    lane = lax.broadcasted_iota(jnp.int32, (Q_TILE, lanes), 1)
    for t in range(n_tiles):
        at = slice(t * Q_TILE, (t + 1) * Q_TILE)
        n_keys = (t + 1) * Q_TILE
        q_blk = q_ref[at, :]
        heads_out = []
        for h in range(lanes // head_dim):
            mine = (lane >= h * head_dim) & (lane < (h + 1) * head_dim)
            q_h = jnp.where(mine, q_blk, jnp.zeros((), q_blk.dtype))
            s = lax.dot_general(q_h, k_ref[:n_keys, :], (((1,), (1,)), ((), ())), preferred_element_type=jnp.float32)
            s = s + bias_ref[at, :n_keys]
            top = jnp.max(s, axis=1, keepdims=True)
            e = jnp.exp(s - top)
            total = jnp.sum(e, axis=1, keepdims=True)
            o_h = jnp.dot(e.astype(jnp.bfloat16), v_ref[:n_keys, :], preferred_element_type=jnp.float32)
            heads_out.append(jnp.where(mine, o_h / total, 0.0))
        o_ref[at, :] = sum(heads_out).astype(o_ref.dtype)


def attention(q, k, v, doc_ids, positions, head_dim):
    rows, width = q.shape
    lanes = 128
    meta = jnp.stack([doc_ids, positions])
    head_spec = pl.BlockSpec((rows, lanes), lambda n: (0, n))
    whole = lambda a: pl.BlockSpec(a.shape, lambda n: (0, 0))
    meta_t = meta.T
    return pl.pallas_call(
        functools.partial(attn_kernel, head_dim),
        out_shape=jax.ShapeDtypeStruct((rows, width), jnp.bfloat16),
        grid=(width // lanes,),
        in_specs=[head_spec, head_spec, head_spec, whole(meta), whole(meta_t)],
        out_specs=head_spec,
        scratch_shapes=[pltpu.VMEM((rows, rows), jnp.float32)],
        compiler_params=pltpu.CompilerParams(vmem_limit_bytes=56 * 1024 * 1024),
        cost_estimate=pl.CostEstimate(flops=3 * rows * rows * width, bytes_accessed=8 * rows * width, transcendentals=rows * rows * width // 128),
        name="attention",
    )(q, k, v, meta, meta_t)


def layer(dest_rows, doc_ids, positions, g_attn, w_q, w_k, w_v, w_o, g_mlp, w_gate, w_up, w_down):
    model_dim = dest_rows.shape[1]
    n_heads, head_dim = w_q.shape[1:]
    cos_t, sin_t = rope_tables(positions, head_dim)
    normed = rms_norm(dest_rows, g_attn)
    q, k, v = qkv_proj(normed, w_q, w_k, w_v, cos_t, sin_t)
    attn_heads = attention(q, k, v, doc_ids, positions, head_dim)
    attn_out = jnp.dot(attn_heads, w_o.reshape(n_heads * head_dim, model_dim), preferred_element_type=jnp.float32).astype(jnp.bfloat16)
    resid_mid = (dest_rows.astype(jnp.float32) + attn_out.astype(jnp.float32)).astype(jnp.bfloat16)
    normed_mlp = rms_norm(resid_mid, g_mlp)
    gate_proj = jnp.dot(normed_mlp, w_gate, preferred_element_type=jnp.float32)
    up_proj = jnp.dot(normed_mlp, w_up, preferred_element_type=jnp.float32)
    hidden_act = (jax.nn.silu(gate_proj) * up_proj).astype(jnp.bfloat16)
    down_proj = jnp.dot(hidden_act, w_down, preferred_element_type=jnp.float32).astype(jnp.bfloat16)
    return (resid_mid.astype(jnp.float32) + down_proj.astype(jnp.float32)).astype(jnp.bfloat16)


def relay_tables(group):
    def at(dev, chips_on, flip):
        return (dev // 2 + chips_on) % (group // 2) * 2 + (dev % 2 ^ int(flip))

    relay_of = np.array([[at(i, o, f) for o, f in RELAYS] for i in range(group)])
    source_of = np.array([[at(k, -o, f) for o, f in RELAYS] for k in range(group)])
    residue = np.array([range(len(RELAYS))] * group)
    return relay_of, source_of, residue


def ceil_div(a, b):
    return -((-a) // b)


def pick(table, index, n):
    return jnp.sum(jnp.where(index[:, None] == jnp.arange(n)[None, :], table[None, :], 0), axis=1)


def plan_indices(me, len_ij, tok_perm, n_tok, n_cap, cap1, cap2, relay_of, source_of, residue):
    group, n_relay = relay_of.shape
    off_ij = jnp.cumsum(len_ij, axis=1) - len_ij
    roff_ij = jnp.cumsum(len_ij, axis=0) - len_ij
    res = np.arange(n_relay)
    first = ceil_div(off_ij[:, None, :] - res[None, :, None], n_relay)
    count = ceil_div((off_ij + len_ij)[:, None, :] - res[None, :, None], n_relay) - first
    first_k = first[source_of, residue]
    count_k = count[source_of, residue]
    base_k = jnp.cumsum(count_k, axis=1) - count_k
    end_k = base_k + count_k

    def mine(t):
        return lax.dynamic_index_in_dim(t, me, 0, keepdims=False)

    base_me, end_me, first_me = mine(base_k), mine(end_k), mine(first_k)
    q = jnp.arange(cap2)
    in_m = (q[None, None, :] >= base_me[:, :, None]) & (q[None, None, :] < end_me[:, :, None])
    src = jnp.arange(n_relay)[:, None, None] * cap1 + first_me[:, :, None] + q[None, None, :] - base_me[:, :, None]
    relay_idx = jnp.sum(jnp.where(in_m, src, 0), axis=0).reshape(-1)

    slot = jnp.arange(cap1)
    in_j = (slot[None, None, :] >= first_me[:, :, None]) & (slot[None, None, :] < (first_me + end_me - base_me)[:, :, None])
    back = jnp.arange(group)[None, :, None] * cap2 + base_me[:, :, None] + slot[None, None, :] - first_me[:, :, None]
    relay_back_idx = jnp.sum(jnp.where(in_j, back + 1, 0), axis=1).reshape(-1) - 1

    len_me = lax.dynamic_index_in_dim(len_ij, me, 1, keepdims=False)
    off_me = lax.dynamic_index_in_dim(off_ij, me, 1, keepdims=False)
    roff_me = lax.dynamic_index_in_dim(roff_ij, me, 1, keepdims=False)
    base_ic = jnp.zeros((group, n_relay), jnp.int32)
    base_to_me = lax.dynamic_index_in_dim(base_k, me, 2, keepdims=False)
    first_to_me = lax.dynamic_index_in_dim(first, me, 2, keepdims=False)
    place = np.zeros((group, n_relay), np.int32)
    for k in range(group):
        for m in range(n_relay):
            place[source_of[k, m], residue[k, m]] = k * n_relay + m
    base_ic = base_to_me.reshape(-1)[place]
    table = relay_of * cap2 + base_ic - first_to_me
    u = jnp.arange(n_cap)
    in_i = (u[:, None] >= roff_me[None, :]) & (u[:, None] < (roff_me + len_me)[None, :])
    r_of_u = jnp.sum(jnp.where(in_i, off_me[None, :] + u[:, None] - roff_me[None, :], 0), axis=1)
    i_of_u = jnp.sum(jnp.where(in_i, np.arange(group)[None, :], 0), axis=1)
    c_of_u = lax.rem(r_of_u, n_relay)
    dest_idx = pick(table.reshape(-1), i_of_u * n_relay + c_of_u, group * n_relay) + r_of_u // n_relay

    count_to_me = lax.dynamic_index_in_dim(count_k, me, 2, keepdims=False)
    first_km = lax.dynamic_index_in_dim(first_k, me, 2, keepdims=False)
    in_km = (q[None, None, :] >= base_to_me[:, :, None]) & (q[None, None, :] < (base_to_me + count_to_me)[:, :, None])
    r_km = (first_km[:, :, None] + q[None, None, :] - base_to_me[:, :, None]) * n_relay + residue[:, :, None]
    u_km = r_km + (roff_me - off_me)[source_of][:, :, None]
    dest_back_idx = jnp.sum(jnp.where(in_km, u_km, 0), axis=1).reshape(-1)

    send_idx = jnp.pad(tok_perm, (0, cap1 * n_relay - n_tok)).reshape(cap1, n_relay).T.reshape(-1)
    inv_perm = jnp.argsort(tok_perm)
    final_idx = lax.rem(inv_perm, n_relay) * cap1 + inv_perm // n_relay
    return send_idx, relay_idx, dest_idx, dest_back_idx, relay_back_idx, final_idx


N_TILE = 512
RELAYS = ((0, False), (0, True), (1, False), (1, True), (-1, False), (-1, True))
NEAR_ORDER = (2, 4, 3, 5, 1, 0)
FAR_ORDER = ((2, False), (1, False), (-1, False), (2, True), (1, True), (-1, True), (0, True), (0, False))


def peer(me, group, chips_on, flip):
    n_chips = group // 2
    chip = lax.rem(me // 2 + chips_on + n_chips, n_chips)
    core = lax.rem(me, 2)
    if flip:
        core = 1 - core
    return chip * 2 + core


def build_pick(idx_ref, at, pick_ref, n_src):
    lane = lax.broadcasted_iota(jnp.int32, (at.size, n_src), 1)
    pick_ref[:at.size, :n_src] = (idx_ref[at, :] == lane).astype(jnp.float32).astype(pick_ref.dtype)


def gather_rows(src_ref, pick_ref, dst_ref, dst_at):
    n_src, width = src_ref.shape

    @pl.loop(0, width // N_TILE)
    def _(n):
        cols = pl.ds(pl.multiple_of(n * N_TILE, N_TILE), N_TILE)
        rows = jnp.dot(pick_ref[:dst_at.size, :n_src], src_ref[:, cols], preferred_element_type=jnp.float32)
        dst_ref[dst_at, cols] = rows.astype(dst_ref.dtype)


def hop(src_ref, idx_ref, pick_ref, buf_ref, land_ref, land_local, cap, targets, send_sem, recv_sem):
    copies = []
    for t, (dev, block, slot) in enumerate(targets):
        build_pick(idx_ref, pl.ds(pl.multiple_of(block * cap, 16), cap), pick_ref, src_ref.shape[0])
        if copies:
            copies[-1].start()
        here = pl.ds(t * cap, cap)
        there = pl.ds(pl.multiple_of(slot * cap, 16), cap)
        if dev is None and land_local:
            gather_rows(src_ref, pick_ref, land_ref, there)
            continue
        gather_rows(src_ref, pick_ref, buf_ref, here)
        if dev is None:
            copies.append(pltpu.make_async_copy(buf_ref.at[here, :], land_ref.at[there, :], recv_sem.at[t]))
        else:
            copies.append(pltpu.make_async_remote_copy(
                src_ref=buf_ref.at[here, :],
                dst_ref=land_ref.at[there, :],
                send_sem=send_sem.at[t],
                recv_sem=recv_sem.at[t],
                device_id={'sp': dev},
                device_id_type=pl.DeviceIdType.MESH,
            ))
    if not land_local:
        copies[-1].start()
    for copy in copies:
        copy.wait()


def two_hop_kernel(group, near_first, cap_a, cap_b, src_ref, idx_a_ref, idx_b_ref, out_ref, pick_ref, buf_a_ref, mid_ref, buf_b_ref, sem_a_send, sem_a_recv, sem_b_send, sem_b_recv):
    me = lax.axis_index('sp')
    barrier = pltpu.get_barrier_semaphore()
    for other in range(1, group):
        pl.semaphore_signal(barrier, inc=1, device_id={'sp': lax.rem(me + other, group)}, device_id_type=pl.DeviceIdType.MESH)
    pl.semaphore_wait(barrier, group - 1)
    near = []
    sign = 1 if near_first else -1
    for block in NEAR_ORDER:
        chips_on, flip = RELAYS[block]
        dev = None if (chips_on == 0 and not flip) else peer(me, group, sign * chips_on, flip)
        near.append((dev, block, block))
    far = []
    for chips_on, flip in FAR_ORDER:
        dev = peer(me, group, chips_on, flip)
        far.append((None if (chips_on == 0 and not flip) else dev, dev, me))
    first, second = (near, far) if near_first else (far, near)
    hop(src_ref, idx_a_ref, pick_ref, buf_a_ref, mid_ref, True, cap_a, first, sem_a_send, sem_a_recv)
    hop(mid_ref, idx_b_ref, pick_ref, buf_b_ref, out_ref, False, cap_b, second, sem_b_send, sem_b_recv)


def two_hop(src, idx_a, idx_b, group, near_first, collective_id):
    n_src, width = src.shape
    n_a = len(RELAYS) if near_first else group
    n_b = group if near_first else len(RELAYS)
    rows_a, rows_b = idx_a.shape[0], idx_b.shape[0]
    vmem = pl.BlockSpec(memory_space=pltpu.VMEM)
    return pl.pallas_call(
        functools.partial(two_hop_kernel, group, near_first, rows_a // n_a, rows_b // n_b),
        out_shape=jax.ShapeDtypeStruct((rows_b, width), src.dtype),
        in_specs=[vmem, vmem, vmem],
        out_specs=pl.BlockSpec(memory_space=pl.ANY),
        scratch_shapes=[
            pltpu.VMEM((max(rows_a // n_a, rows_b // n_b), max(n_src, rows_a)), src.dtype),
            pltpu.VMEM((rows_a, width), src.dtype),
            pltpu.VMEM((rows_a, width), src.dtype),
            pltpu.VMEM((rows_b, width), src.dtype),
            pltpu.SemaphoreType.DMA((n_a,)),
            pltpu.SemaphoreType.DMA((n_a,)),
            pltpu.SemaphoreType.DMA((n_b,)),
            pltpu.SemaphoreType.DMA((n_b,)),
        ],
        compiler_params=pltpu.CompilerParams(collective_id=collective_id, has_side_effects=True, vmem_limit_bytes=60 * 1024 * 1024),
        name="two_hop_out" if near_first else "two_hop_back",
    )(src, idx_a[:, None], idx_b[:, None])


def solution(mesh):
    row_spec = P(('dp', 'sp'), None)
    vec_spec = P(('dp', 'sp'))
    rep_spec = P()

    def per_device(hidden, tok_perm, send_off, send_len, recv_off, recv_len, recv_doc, recv_pos, g_attn, w_q, w_k, w_v, w_o, g_mlp, w_gate, w_up, w_down):
        n_tok, model_dim = hidden.shape
        n_cap = recv_doc.shape[0]
        group = send_off.shape[0]
        relay_of, source_of, residue = relay_tables(group)
        n_relay = relay_of.shape[1]
        cap1 = -(-n_tok // n_relay)
        cap2 = -(-(n_cap + n_relay * (n_relay - 1)) // n_relay)
        cap2 = -(-cap2 // 16) * 16
        me = lax.axis_index('sp')
        len_ij = lax.all_gather(send_len, 'sp')
        send_idx, relay_idx, dest_idx, dest_back_idx, relay_back_idx, final_idx = plan_indices(
            me, len_ij, tok_perm, n_tok, n_cap, cap1, cap2, relay_of, source_of, residue)

        def take(rows, index):
            return rows.at[index].get(mode='promise_in_bounds')

        out_at_dest = two_hop(hidden, send_idx, relay_idx, group, True, 0)
        dest_rows = take(out_at_dest, dest_idx)
        out_rows = layer(dest_rows, recv_doc, recv_pos, g_attn, w_q, w_k, w_v, w_o, g_mlp, w_gate, w_up, w_down)
        src_back = two_hop(out_rows, dest_back_idx, relay_back_idx, group, False, 1)
        return take(src_back, final_idx)

    return jax.shard_map(per_device, mesh=mesh, in_specs=(row_spec,) + (vec_spec,) * 7 + (rep_spec,) * 9, out_specs=row_spec, check_vma=False)
```

```python
import functools

import jax
import jax.numpy as jnp
import numpy as np
from jax import lax
from jax.experimental import pallas as pl
from jax.experimental.pallas import tpu as pltpu
from jax.sharding import PartitionSpec as P

ROPE_BASE = 500000.0
NORM_EPS = 1e-5
Q_TILE = 256
QKV_TILE = 256


def rms_norm(rows_in, gain_vec):
    rows_f = rows_in.astype(jnp.float32)
    inv_rms = lax.rsqrt(jnp.mean(rows_f * rows_f, axis=-1, keepdims=True) + NORM_EPS)
    return (rows_f * inv_rms * gain_vec.astype(jnp.float32)).astype(jnp.bfloat16)


def rope_tables(positions, head_dim):
    half = head_dim // 2
    inv_freq = jnp.power(jnp.float32(ROPE_BASE), -2.0 * jnp.arange(half, dtype=jnp.float32) / head_dim)
    angles = positions.astype(jnp.float32)[:, None] * inv_freq[None, :]
    cos_t = jnp.cos(angles)
    sin_t = jnp.sin(angles)
    return jnp.concatenate([cos_t] * 4, axis=1), jnp.concatenate([-sin_t, sin_t] * 2, axis=1)


def qkv_proj(normed, w_q, w_k, w_v, cos_t, sin_t):
    rows, model_dim = normed.shape
    n_heads, head_dim = w_q.shape[1:]
    width = n_heads * head_dim
    w_all = [w.transpose(1, 2, 0).reshape(width, model_dim) for w in (w_q, w_k, w_v)]
    outs = []
    for kind, w in enumerate(w_all):
        outs.append(pl.pallas_call(
            functools.partial(qkv_one, head_dim, kind),
            out_shape=jax.ShapeDtypeStruct((rows, width), jnp.bfloat16),
            grid=(width // QKV_TILE,),
            in_specs=[
                pl.BlockSpec((rows, model_dim), lambda n: (0, 0), pipeline_mode=pl.Buffered(1)),
                pl.BlockSpec((QKV_TILE, model_dim), lambda n: (n, 0)),
                pl.BlockSpec(cos_t.shape, lambda n: (0, 0), pipeline_mode=pl.Buffered(1)),
                pl.BlockSpec(sin_t.shape, lambda n: (0, 0), pipeline_mode=pl.Buffered(1)),
            ],
            out_specs=pl.BlockSpec((rows, QKV_TILE), lambda n: (0, n)),
            compiler_params=pltpu.CompilerParams(vmem_limit_bytes=48 * 1024 * 1024),
            cost_estimate=pl.CostEstimate(flops=2 * rows * model_dim * width, bytes_accessed=2 * (2 * rows * model_dim + model_dim * width), transcendentals=0),
            name="qkv",
        )(normed, w, cos_t, sin_t))
    return outs


def qkv_one(head_dim, kind, h_ref, w_ref, cos_ref, sin_ref, o_ref):
    lanes = cos_ref.shape[1]
    half = head_dim // 2
    acc = lax.dot_general(h_ref[...], w_ref[...], (((1,), (1,)), ((), ())), preferred_element_type=jnp.float32)
    if kind == 2:
        o_ref[...] = acc.astype(o_ref.dtype)
        return
    first = lax.rem(lax.broadcasted_iota(jnp.int32, (1, lanes), 1), head_dim) < half
    for b in range(o_ref.shape[1] // lanes):
        x = acc[:, b * lanes:(b + 1) * lanes]
        swapped = jnp.where(first, pltpu.roll(x, lanes - half, 1), pltpu.roll(x, half, 1))
        rot = x * cos_ref[...] + swapped * sin_ref[...]
        if kind == 0:
            rot = rot * (head_dim ** -0.5)
        o_ref[:, b * lanes:(b + 1) * lanes] = rot.astype(o_ref.dtype)


def attn_kernel(head_dim, q_ref, k_ref, v_ref, meta_row_ref, meta_col_ref, o_ref, bias_ref):
    rows, lanes = q_ref.shape
    n_tiles = rows // Q_TILE

    @pl.when(pl.program_id(0) == 0)
    def _():
        for t in range(n_tiles):
            at = slice(t * Q_TILE, (t + 1) * Q_TILE)
            n_keys = (t + 1) * Q_TILE
            ok = (meta_col_ref[at, 0:1] == meta_row_ref[0:1, :n_keys]) & (meta_row_ref[1:2, :n_keys] <= meta_col_ref[at, 1:2])
            bias_ref[at, :n_keys] = jnp.where(ok, 0.0, -1e30).astype(jnp.float32)

    low = lax.broadcasted_iota(jnp.int32, (Q_TILE, lanes), 1) < head_dim

    def scores(t):
        q = q_ref[t * Q_TILE:(t + 1) * Q_TILE, :]
        zero = jnp.zeros((), q.dtype)
        both = jnp.concatenate([jnp.where(low, q, zero), jnp.where(low, zero, q)], axis=0)
        return lax.dot_general(both, k_ref[:(t + 1) * Q_TILE, :], (((1,), (1,)), ((), ())), preferred_element_type=jnp.float32)

    def outputs(t, s):
        at = slice(t * Q_TILE, (t + 1) * Q_TILE)
        n_keys = (t + 1) * Q_TILE
        s = s.reshape(2, Q_TILE, n_keys) + bias_ref[at, :n_keys][None]
        e = jnp.exp(s - jnp.max(s, axis=2, keepdims=True))
        total = jnp.sum(e, axis=2, keepdims=True)
        o = jnp.dot(e.astype(jnp.bfloat16).reshape(2 * Q_TILE, n_keys), v_ref[:n_keys, :], preferred_element_type=jnp.float32)
        o = o.reshape(2, Q_TILE, lanes) / total
        o_ref[at, :] = jnp.where(low, o[0], o[1]).astype(o_ref.dtype)

    ahead = scores(0)
    for t in range(n_tiles):
        s = ahead
        if t + 1 < n_tiles:
            ahead = scores(t + 1)
        outputs(t, s)


def attention(q, k, v, doc_ids, positions, head_dim):
    rows, width = q.shape
    lanes = 2 * head_dim
    meta = jnp.stack([doc_ids, positions])
    head_spec = pl.BlockSpec((rows, lanes), lambda n: (0, n))
    whole = lambda a: pl.BlockSpec(a.shape, lambda n: (0, 0))
    meta_t = meta.T
    return pl.pallas_call(
        functools.partial(attn_kernel, head_dim),
        out_shape=jax.ShapeDtypeStruct((rows, width), jnp.bfloat16),
        grid=(width // lanes,),
        in_specs=[head_spec, head_spec, head_spec, whole(meta), whole(meta_t)],
        out_specs=head_spec,
        scratch_shapes=[pltpu.VMEM((rows, rows), jnp.float32)],
        compiler_params=pltpu.CompilerParams(vmem_limit_bytes=56 * 1024 * 1024),
        cost_estimate=pl.CostEstimate(flops=3 * rows * rows * width, bytes_accessed=8 * rows * width, transcendentals=rows * rows * width // 128),
        name="attention",
    )(q, k, v, meta, meta_t)


def attn_layer(dest_rows, doc_ids, positions, g_attn, w_q, w_k, w_v, w_o):
    model_dim = dest_rows.shape[1]
    n_heads, head_dim = w_q.shape[1:]
    cos_t, sin_t = rope_tables(positions, head_dim)
    normed = rms_norm(dest_rows, g_attn)
    q, k, v = qkv_proj(normed, w_q, w_k, w_v, cos_t, sin_t)
    attn_heads = attention(q, k, v, doc_ids, positions, head_dim)
    attn_out = jnp.dot(attn_heads, w_o.reshape(n_heads * head_dim, model_dim), preferred_element_type=jnp.float32).astype(jnp.bfloat16)
    return (dest_rows.astype(jnp.float32) + attn_out.astype(jnp.float32)).astype(jnp.bfloat16)


def relay_tables(group):
    def at(dev, chips_on, flip):
        return (dev // 2 + chips_on) % (group // 2) * 2 + (dev % 2 ^ int(flip))

    relay_of = np.array([[at(i, o, f) for o, f in RELAYS] for i in range(group)])
    source_of = np.array([[at(k, -o, f) for o, f in RELAYS] for k in range(group)])
    return relay_of, source_of


def ceil_div(a, b):
    return -((-a) // b)


def pick(table, index, n):
    return jnp.sum(jnp.where(index[:, None] == jnp.arange(n)[None, :], table[None, :], 0), axis=1)


def run_tables(len_ij, n_classes):
    off_ij = jnp.cumsum(len_ij, axis=1) - len_ij
    res = np.arange(n_classes)
    first = ceil_div(off_ij[:, None, :] - res[None, :, None], n_classes)
    count = ceil_div((off_ij + len_ij)[:, None, :] - res[None, :, None], n_classes) - first
    return first, count


def out_indices(me, len_ij, tok_perm, n_cap, cap1, cap2, relay_of, source_of):
    group, n_relay = relay_of.shape
    off_ij = jnp.cumsum(len_ij, axis=1) - len_ij
    roff_ij = jnp.cumsum(len_ij, axis=0) - len_ij
    first, count = run_tables(len_ij, n_relay)
    res = np.arange(n_relay)
    first_k = first[source_of, res]
    count_k = count[source_of, res]
    base_k = jnp.cumsum(count_k, axis=1) - count_k

    def mine(t, axis=0):
        return lax.dynamic_index_in_dim(t, me, axis, keepdims=False)

    base_me, count_me, first_me = mine(base_k), mine(count_k), mine(first_k)
    q = jnp.arange(cap2)
    in_m = (q >= base_me[:, :, None]) & (q < (base_me + count_me)[:, :, None])
    src = np.arange(n_relay)[:, None, None] * cap1 + first_me[:, :, None] + q - base_me[:, :, None]
    relay_idx = jnp.sum(jnp.where(in_m, src, 0), axis=0).reshape(-1)

    len_me, off_me, roff_me = mine(len_ij, 1), mine(off_ij, 1), mine(roff_ij, 1)
    base_to_me, first_to_me = mine(base_k, 2), mine(first, 2)
    place = np.zeros((group, n_relay), np.int32)
    place[source_of, res] = np.arange(group)[:, None] * n_relay + res
    table = relay_of * cap2 + base_to_me.reshape(-1)[place] - first_to_me
    u = jnp.arange(n_cap)
    in_i = (u[:, None] >= roff_me[None, :]) & (u[:, None] < (roff_me + len_me)[None, :])
    r_of_u = jnp.sum(jnp.where(in_i, off_me[None, :] + u[:, None] - roff_me[None, :], 0), axis=1)
    i_of_u = jnp.sum(jnp.where(in_i, np.arange(group)[None, :], 0), axis=1)
    dest_idx = pick(table.reshape(-1), i_of_u * n_relay + lax.rem(r_of_u, n_relay), group * n_relay) + r_of_u // n_relay

    send_idx = jnp.pad(tok_perm, (0, cap1 * n_relay - tok_perm.shape[0])).reshape(cap1, n_relay).T.reshape(-1)
    return send_idx, relay_idx, dest_idx


def back_indices(me, len_ij, tok_perm, n_rows, cap1, cap2, source_of, n_chunks):
    group, n_relay = source_of.shape
    n_classes = n_relay * n_chunks
    off_ij = jnp.cumsum(len_ij, axis=1) - len_ij
    roff_ij = jnp.cumsum(len_ij, axis=0) - len_ij
    first, count = run_tables(len_ij, n_classes)
    cls = (np.arange(n_chunks)[:, None] * n_relay + np.arange(n_relay)[None, :])
    first_k = first[source_of[:, None, :], cls[None]]
    count_k = count[source_of[:, None, :], cls[None]]
    base_k = jnp.cumsum(count_k, axis=2) - count_k

    def mine(t, axis=0):
        return lax.dynamic_index_in_dim(t, me, axis, keepdims=False)

    cnt = mine(count_k, 3).transpose(1, 0, 2).reshape(n_chunks, -1)
    fst = mine(first_k, 3).transpose(1, 0, 2).reshape(n_chunks, -1)
    start = jnp.cumsum(cnt, axis=1) - cnt
    shift = jnp.broadcast_to(cls[:, None, :] + mine(roff_ij - off_ij, 1)[source_of][None], (n_chunks, group, n_relay)).reshape(n_chunks, -1)
    p = jnp.arange(n_rows)
    in_run = (p >= start[:, :, None]) & (p < (start + cnt)[:, :, None])
    u_of_p = (fst[:, :, None] + p - start[:, :, None]) * n_classes + shift[:, :, None]
    chunk_idx = jnp.sum(jnp.where(in_run, u_of_p + 1, 0), axis=1).reshape(-1) - 1

    n_k = jnp.sum(cnt.reshape(n_chunks, group, n_relay), axis=2)
    start_k = jnp.cumsum(n_k, axis=1) - n_k
    q = jnp.arange(cap2)
    far_idx = jnp.where(q < n_k[:, :, None], start_k[:, :, None] + q, -1).reshape(-1)

    base_me, count_me, first_me = mine(base_k), mine(count_k), mine(first_k)
    slot = jnp.arange(cap1)
    in_j = (slot >= first_me[..., None]) & (slot < (first_me + count_me)[..., None])
    back = np.arange(group)[:, None] * cap2 + base_me[..., None] + slot - first_me[..., None]
    near_idx = jnp.sum(jnp.where(in_j, back + 1, 0), axis=2).reshape(-1) - 1

    inv_perm = jnp.argsort(tok_perm)
    group_no = inv_perm // n_relay
    final_idx = (lax.rem(group_no, n_chunks) * n_relay + lax.rem(inv_perm, n_relay)) * cap1 + group_no // n_chunks
    return chunk_idx, far_idx, near_idx, final_idx


N_TILE = 512
RELAYS = ((0, False), (0, True), (1, False), (1, True), (-1, False), (-1, True))
NEAR_ORDER = (2, 4, 3, 5, 1, 0)
FAR_ORDER = ((2, False), (1, False), (-1, False), (2, True), (1, True), (-1, True), (0, True), (0, False))


def peer(me, group, chips_on, flip):
    n_chips = group // 2
    chip = lax.rem(me // 2 + chips_on + n_chips, n_chips)
    core = lax.rem(me, 2)
    if flip:
        core = 1 - core
    return chip * 2 + core


def row_block(n, most):
    return max(d for d in range(16, most + 1, 16) if n % d == 0)


def build_pick(idx_ref, at, pick_ref, n_src):
    block = row_block(at.size, 288)

    @pl.loop(0, at.size // block)
    def _(b):
        off = pl.multiple_of(b * block, 16)
        lane = lax.broadcasted_iota(jnp.int32, (block, n_src), 1)
        hit = idx_ref[pl.ds(pl.multiple_of(at.start + off, 16), block), :] == lane
        pick_ref[pl.ds(off, block), :n_src] = hit.astype(jnp.float32).astype(pick_ref.dtype)


def gather_rows(src_ref, pick_ref, dst_ref, dst_at):
    n_src, width = src_ref.shape

    @pl.loop(0, width // N_TILE)
    def _(n):
        cols = pl.ds(pl.multiple_of(n * N_TILE, N_TILE), N_TILE)
        rows = jnp.dot(pick_ref[:dst_at.size, :n_src], src_ref[:, cols], preferred_element_type=jnp.float32)
        dst_ref[dst_at, cols] = rows.astype(dst_ref.dtype)


def hop(src_ref, idx_ref, pick_ref, buf_ref, land_ref, land_local, cap, targets, send_sem, recv_sem):
    copies = []
    for t, (dev, block, slot) in enumerate(targets):
        build_pick(idx_ref, pl.ds(pl.multiple_of(block * cap, 16), cap), pick_ref, src_ref.shape[0])
        if copies:
            copies[-1].start()
        here = pl.ds(t * cap, cap)
        there = pl.ds(pl.multiple_of(slot * cap, 16), cap)
        if dev is None and land_local:
            gather_rows(src_ref, pick_ref, land_ref, there)
            continue
        gather_rows(src_ref, pick_ref, buf_ref, here)
        if dev is None:
            copies.append(pltpu.make_async_copy(buf_ref.at[here, :], land_ref.at[there, :], recv_sem.at[t]))
        else:
            copies.append(pltpu.make_async_remote_copy(
                src_ref=buf_ref.at[here, :],
                dst_ref=land_ref.at[there, :],
                send_sem=send_sem.at[t],
                recv_sem=recv_sem.at[t],
                device_id={'sp': dev},
                device_id_type=pl.DeviceIdType.MESH,
            ))
    if not land_local:
        copies[-1].start()
    for copy in copies:
        copy.wait()


def two_hop_kernel(group, near_first, cap_a, cap_b, src_ref, idx_a_ref, idx_b_ref, out_ref, pick_ref, buf_a_ref, mid_ref, buf_b_ref, sem_a_send, sem_a_recv, sem_b_send, sem_b_recv):
    me = lax.axis_index('sp')
    barrier = pltpu.get_barrier_semaphore()
    for other in range(1, group):
        pl.semaphore_signal(barrier, inc=1, device_id={'sp': lax.rem(me + other, group)}, device_id_type=pl.DeviceIdType.MESH)
    pl.semaphore_wait(barrier, group - 1)
    near = []
    sign = 1 if near_first else -1
    for block in NEAR_ORDER:
        chips_on, flip = RELAYS[block]
        dev = None if (chips_on == 0 and not flip) else peer(me, group, sign * chips_on, flip)
        near.append((dev, block, block))
    far = []
    for chips_on, flip in FAR_ORDER:
        dev = peer(me, group, chips_on, flip)
        far.append((None if (chips_on == 0 and not flip) else dev, dev, me))
    first, second = (near, far) if near_first else (far, near)
    hop(src_ref, idx_a_ref, pick_ref, buf_a_ref, mid_ref, True, cap_a, first, sem_a_send, sem_a_recv)
    hop(mid_ref, idx_b_ref, pick_ref, buf_b_ref, out_ref, False, cap_b, second, sem_b_send, sem_b_recv)


def two_hop(src, idx_a, idx_b, group, near_first, collective_id):
    n_src, width = src.shape
    n_a = len(RELAYS) if near_first else group
    n_b = group if near_first else len(RELAYS)
    rows_a, rows_b = idx_a.shape[0], idx_b.shape[0]
    vmem = pl.BlockSpec(memory_space=pltpu.VMEM)
    return pl.pallas_call(
        functools.partial(two_hop_kernel, group, near_first, rows_a // n_a, rows_b // n_b),
        out_shape=jax.ShapeDtypeStruct((rows_b, width), src.dtype),
        in_specs=[vmem, vmem, vmem],
        out_specs=pl.BlockSpec(memory_space=pl.ANY),
        scratch_shapes=[
            pltpu.VMEM((max(rows_a // n_a, rows_b // n_b), max(n_src, rows_a)), src.dtype),
            pltpu.VMEM((rows_a, width), src.dtype),
            pltpu.VMEM((rows_a, width), src.dtype),
            pltpu.VMEM((rows_b, width), src.dtype),
            pltpu.SemaphoreType.DMA((n_a,)),
            pltpu.SemaphoreType.DMA((n_a,)),
            pltpu.SemaphoreType.DMA((n_b,)),
            pltpu.SemaphoreType.DMA((n_b,)),
        ],
        compiler_params=pltpu.CompilerParams(collective_id=collective_id, has_side_effects=True, vmem_limit_bytes=60 * 1024 * 1024),
        name="two_hop_out" if near_first else "two_hop_back",
    )(src, idx_a[:, None], idx_b[:, None])


FF_TILE = 512
BACK_CHUNKS = 3


def mlp_back_kernel(group, n_chunks, cap_far, cap_near, z_ref, gain_ref, chunk_idx_ref, far_idx_ref, near_idx_ref, wg_ref, wu_ref, wd_ref, out_ref,
                    pick_ref, pick2_ref, zo_ref, h2_ref, acc_ref, buf_ref, mid_ref, far_send, far_recv, near_send, near_recv):
    h = pl.program_id(0)
    f = pl.program_id(1)
    last_f = pl.num_programs(1) - 1
    n_rows = h2_ref.shape[0]
    block = row_block(n_rows, 80)
    width = z_ref.shape[1]
    n_far = group * cap_far
    n_near = len(RELAYS) * cap_near
    me = lax.axis_index('sp')

    def far_copies(c):
        copies = []
        for t, (chips_on, flip) in enumerate(FAR_ORDER):
            if chips_on == 0 and not flip:
                continue
            dev = peer(me, group, chips_on, flip)
            copies.append(pltpu.make_async_remote_copy(
                src_ref=buf_ref.at[pl.ds(pl.multiple_of(dev * cap_far, 16), cap_far), :],
                dst_ref=mid_ref.at[pl.ds(pl.multiple_of(c * n_far + me * cap_far, 16), cap_far), :],
                send_sem=far_send.at[c, t], recv_sem=far_recv.at[c, t],
                device_id={'sp': dev}, device_id_type=pl.DeviceIdType.MESH))
        return copies

    def near_copies(c):
        copies = []
        for t in NEAR_ORDER:
            chips_on, flip = RELAYS[t]
            src = buf_ref.at[pl.ds(t * cap_near, cap_near), :]
            dst = out_ref.at[pl.ds(c * n_near + t * cap_near, cap_near), :]
            if chips_on == 0 and not flip:
                copies.append(pltpu.make_async_copy(src, dst, near_recv.at[c, t]))
            else:
                copies.append(pltpu.make_async_remote_copy(
                    src_ref=src, dst_ref=dst, send_sem=near_send.at[c, t], recv_sem=near_recv.at[c, t],
                    device_id={'sp': peer(me, group, -chips_on, flip)}, device_id_type=pl.DeviceIdType.MESH))
        return copies

    def start_far(c):
        build_pick(far_idx_ref, pl.ds(c * n_far, n_far), pick_ref, n_rows)
        gather_rows(zo_ref.at[pl.ds(c * n_rows, n_rows), :], pick_ref, buf_ref, pl.ds(0, n_far))
        build_pick(near_idx_ref, pl.ds(c * n_near, n_near), pick2_ref, n_far)
        for copy in far_copies(c):
            copy.start()
        own = pl.multiple_of(me * cap_far, 16)
        mid_ref[pl.ds(pl.multiple_of(c * n_far + own, 16), cap_far), :] = buf_ref[pl.ds(own, cap_far), :]

    def start_near(c):
        for copy in far_copies(c):
            copy.wait()
        gather_rows(mid_ref.at[pl.ds(c * n_far, n_far), :], pick2_ref, buf_ref, pl.ds(0, n_near))
        for copy in near_copies(c):
            copy.start()

    def end_near(c):
        for copy in near_copies(c):
            copy.wait()

    @pl.when((h == 0) & (f == 0))
    def _():
        barrier = pltpu.get_barrier_semaphore()
        for other in range(1, group):
            pl.semaphore_signal(barrier, inc=1, device_id={'sp': lax.rem(me + other, group)}, device_id_type=pl.DeviceIdType.MESH)
        pl.semaphore_wait(barrier, group - 1)

    for c in range(n_chunks):
        zo = zo_ref.at[pl.ds(c * n_rows, n_rows), :]

        @pl.when((h == c) & (f == 0))
        def _():
            build_pick(chunk_idx_ref, pl.ds(c * n_rows, n_rows), pick_ref, z_ref.shape[0])
            gather_rows(z_ref, pick_ref, zo, pl.ds(0, n_rows))
            gain = gain_ref[...].astype(jnp.float32)

            @pl.loop(0, n_rows // block)
            def _(b):
                at = pl.ds(pl.multiple_of(b * block, 16), block)
                rows_f = zo[at, :].astype(jnp.float32)
                inv_rms = lax.rsqrt(jnp.mean(rows_f * rows_f, axis=-1, keepdims=True) + NORM_EPS)
                h2_ref[at, :] = (rows_f * inv_rms * gain).astype(h2_ref.dtype)
                acc_ref[at, :] = jnp.zeros((block, width), jnp.float32)

        if c > 0:
            @pl.when((h == c) & (f == (last_f + 1) // 2))
            def _():
                start_near(c - 1)

    gate = jnp.dot(h2_ref[...], wg_ref[...], preferred_element_type=jnp.float32)
    up = jnp.dot(h2_ref[...], wu_ref[...], preferred_element_type=jnp.float32)
    act = (gate * jax.nn.sigmoid(gate) * up).astype(jnp.bfloat16)
    acc_ref[...] += jnp.dot(act, wd_ref[...], preferred_element_type=jnp.float32)

    for c in range(n_chunks):
        zo = zo_ref.at[pl.ds(c * n_rows, n_rows), :]

        @pl.when((h == c) & (f == last_f))
        def _():
            if c > 0:
                end_near(c - 1)

            @pl.loop(0, n_rows // block)
            def _(b):
                at = pl.ds(pl.multiple_of(b * block, 16), block)
                down = acc_ref[at, :].astype(jnp.bfloat16).astype(jnp.float32)
                zo[at, :] = (zo[at, :].astype(jnp.float32) + down).astype(zo_ref.dtype)

            start_far(c)
            if c == n_chunks - 1:
                start_near(c)
                end_near(c)


def mlp_back(z, gain, chunk_idx, far_idx, near_idx, w_gate, w_up, w_down, group, n_rows, cap_far, cap_near, collective_id):
    n_src, width = z.shape
    ff = w_gate.shape[1]
    n_chunks = BACK_CHUNKS
    n_far, n_near = group * cap_far, len(RELAYS) * cap_near
    whole = lambda shape: pl.BlockSpec(shape, lambda h, f: (0, 0), pipeline_mode=pl.Buffered(1))
    return pl.pallas_call(
        functools.partial(mlp_back_kernel, group, n_chunks, cap_far, cap_near),
        out_shape=jax.ShapeDtypeStruct((n_chunks * n_near, width), z.dtype),
        grid=(n_chunks, ff // FF_TILE),
        in_specs=[
            whole(z.shape), whole((1, width)), whole((n_chunks * n_rows, 1)), whole((n_chunks * n_far, 1)), whole((n_chunks * n_near, 1)),
            pl.BlockSpec((width, FF_TILE), lambda h, f: (0, f)),
            pl.BlockSpec((width, FF_TILE), lambda h, f: (0, f)),
            pl.BlockSpec((FF_TILE, width), lambda h, f: (f, 0)),
        ],
        out_specs=pl.BlockSpec(memory_space=pl.ANY),
        scratch_shapes=[
            pltpu.VMEM((max(n_rows, n_far), max(n_src, n_rows)), z.dtype),
            pltpu.VMEM((n_near, n_far), z.dtype),
            pltpu.VMEM((n_chunks * n_rows, width), z.dtype),
            pltpu.VMEM((n_rows, width), z.dtype),
            pltpu.VMEM((n_rows, width), jnp.float32),
            pltpu.VMEM((max(n_far, n_near), width), z.dtype),
            pltpu.VMEM((n_chunks * n_far, width), z.dtype),
            pltpu.SemaphoreType.DMA((n_chunks, group)),
            pltpu.SemaphoreType.DMA((n_chunks, group)),
            pltpu.SemaphoreType.DMA((n_chunks, len(RELAYS))),
            pltpu.SemaphoreType.DMA((n_chunks, len(RELAYS))),
        ],
        compiler_params=pltpu.CompilerParams(collective_id=collective_id, has_side_effects=True, vmem_limit_bytes=63 * 1024 * 1024,
                                             dimension_semantics=("arbitrary", "arbitrary")),
        name="mlp_back",
    )(z, gain.reshape(1, width), chunk_idx[:, None], far_idx[:, None], near_idx[:, None], w_gate, w_up, w_down)


def solution(mesh):
    row_spec = P(('dp', 'sp'), None)
    vec_spec = P(('dp', 'sp'))
    rep_spec = P()

    def per_device(hidden, tok_perm, send_off, send_len, recv_off, recv_len, recv_doc, recv_pos, g_attn, w_q, w_k, w_v, w_o, g_mlp, w_gate, w_up, w_down):
        n_tok, model_dim = hidden.shape
        n_cap = recv_doc.shape[0]
        group = send_off.shape[0]
        relay_of, source_of = relay_tables(group)
        n_relay = relay_of.shape[1]
        round_up = lambda n, unit: -(-n // unit) * unit
        cap1 = round_up(-(-n_tok // n_relay), 16)
        cap2 = round_up((n_cap + n_relay * (n_relay - 1)) // n_relay, 16)
        n_classes = n_relay * BACK_CHUNKS
        cap1_back = round_up(-(-n_tok // n_classes), 16)
        cap2_back = round_up((n_cap + n_relay * (n_classes - 1)) // n_classes, 16)
        n_rows = round_up(-(-(n_cap + group * n_relay * (BACK_CHUNKS - 1)) // BACK_CHUNKS), 16)
        me = lax.axis_index('sp')
        len_ij = lax.all_gather(send_len, 'sp')
        send_idx, relay_idx, dest_idx = out_indices(me, len_ij, tok_perm, n_cap, cap1, cap2, relay_of, source_of)
        chunk_idx, far_idx, near_idx, final_idx = back_indices(me, len_ij, tok_perm, n_rows, cap1_back, cap2_back, source_of, BACK_CHUNKS)

        def take(rows, index):
            return rows.at[index].get(mode='promise_in_bounds')

        at_dest = two_hop(hidden, send_idx, relay_idx, group, True, 0)
        z = attn_layer(take(at_dest, dest_idx), recv_doc, recv_pos, g_attn, w_q, w_k, w_v, w_o)
        src_back = mlp_back(z, g_mlp, chunk_idx, far_idx, near_idx, w_gate, w_up, w_down, group, n_rows, cap2_back, cap1_back, 1)
        return take(src_back, final_idx)

    return jax.shard_map(per_device, mesh=mesh, in_specs=(row_spec,) + (vec_spec,) * 7 + (rep_spec,) * 9, out_specs=row_spec, check_vma=False)
```

```python
import functools

import jax
import jax.numpy as jnp
import numpy as np
from jax import lax
from jax.experimental import pallas as pl
from jax.experimental.pallas import tpu as pltpu
from jax.sharding import PartitionSpec as P

ROPE_BASE = 500000.0
NORM_EPS = 1e-5
Q_TILE = 256
QKV_TILE = 256


def rope_tables(positions, head_dim):
    half = head_dim // 2
    inv_freq = jnp.power(jnp.float32(ROPE_BASE), -2.0 * jnp.arange(half, dtype=jnp.float32) / head_dim)
    angles = positions.astype(jnp.float32)[:, None] * inv_freq[None, :]
    cos_t = jnp.cos(angles)
    sin_t = jnp.sin(angles)
    return jnp.concatenate([cos_t] * 4, axis=1), jnp.concatenate([-sin_t, sin_t] * 2, axis=1)


def qkv_kernel(head_dim, blocks_ref, idx_ref, gain_ref, cos_ref, sin_ref, wq_ref, wk_ref, wv_ref, r_ref, q_ref, k_ref, v_ref, pick_ref, h_ref):
    n = pl.program_id(0)
    n_each = pl.num_programs(0) // 3
    rows = r_ref.shape[0]
    lanes = cos_ref.shape[1]
    half = head_dim // 2

    @pl.when(n == 0)
    def _():
        build_pick(idx_ref, pl.ds(0, rows), pick_ref, blocks_ref.shape[0])
        gather_rows(blocks_ref, pick_ref, r_ref, pl.ds(0, rows))
        norm_rows(r_ref, gain_ref, h_ref)

    for kind, (w_ref, o_ref) in enumerate(((wq_ref, q_ref), (wk_ref, k_ref), (wv_ref, v_ref))):
        @pl.when(n // n_each == kind)
        def _():
            acc = lax.dot_general(h_ref[...], w_ref[...], (((1,), (1,)), ((), ())), preferred_element_type=jnp.float32)
            if kind == 2:
                o_ref[...] = acc.astype(o_ref.dtype)
                return
            first = lax.rem(lax.broadcasted_iota(jnp.int32, (1, lanes), 1), head_dim) < half
            for b in range(o_ref.shape[1] // lanes):
                x = acc[:, b * lanes:(b + 1) * lanes]
                swapped = jnp.where(first, pltpu.roll(x, lanes - half, 1), pltpu.roll(x, half, 1))
                rot = x * cos_ref[...] + swapped * sin_ref[...]
                if kind == 0:
                    rot = rot * (head_dim ** -0.5)
                o_ref[:, b * lanes:(b + 1) * lanes] = rot.astype(o_ref.dtype)


def qkv_proj(blocks, dest_idx, gain, w_q, w_k, w_v, cos_t, sin_t):
    rows = dest_idx.shape[0]
    model_dim = blocks.shape[1]
    n_heads, head_dim = w_q.shape[1:]
    width = n_heads * head_dim
    n_each = width // QKV_TILE
    w_all = [w.transpose(1, 2, 0).reshape(width, model_dim) for w in (w_q, w_k, w_v)]
    once = lambda shape: pl.BlockSpec(shape, lambda n: (0, 0), pipeline_mode=pl.Buffered(1))
    tile = lambda kind: (lambda n: jnp.clip(n - kind * n_each, 0, n_each - 1))
    return pl.pallas_call(
        functools.partial(qkv_kernel, head_dim),
        out_shape=[jax.ShapeDtypeStruct((rows, model_dim), blocks.dtype)] + [jax.ShapeDtypeStruct((rows, width), blocks.dtype)] * 3,
        grid=(3 * n_each,),
        in_specs=[once(blocks.shape), once((rows, 1)), once((1, model_dim)), once(cos_t.shape), once(sin_t.shape)]
        + [pl.BlockSpec((QKV_TILE, model_dim), lambda n, t=tile(kind): (t(n), 0)) for kind in range(3)],
        out_specs=[once((rows, model_dim))] + [pl.BlockSpec((rows, QKV_TILE), lambda n, t=tile(kind): (0, t(n))) for kind in range(3)],
        scratch_shapes=[pltpu.VMEM((rows, blocks.shape[0]), blocks.dtype), pltpu.VMEM((rows, model_dim), blocks.dtype)],
        compiler_params=pltpu.CompilerParams(vmem_limit_bytes=56 * 1024 * 1024, dimension_semantics=("arbitrary",)),
        cost_estimate=pl.CostEstimate(flops=6 * rows * model_dim * width, bytes_accessed=6 * model_dim * width, transcendentals=0),
        name="qkv",
    )(blocks, dest_idx[:, None], gain.reshape(1, model_dim), cos_t, sin_t, *w_all)


def attn_kernel(head_dim, n_parts, q_ref, *refs):
    k_parts, v_parts = refs[:n_parts], refs[n_parts:2 * n_parts]
    meta_row_ref, meta_col_ref, o_ref, bias_ref, k_ref, v_ref = refs[2 * n_parts:]
    rows, lanes = q_ref.shape
    n_tiles = rows // Q_TILE
    before = k_ref.shape[0] - rows

    @pl.when(pl.program_id(0) == 0)
    def _():
        for t in range(n_tiles):
            at = slice(t * Q_TILE, (t + 1) * Q_TILE)
            n_keys = before + (t + 1) * Q_TILE
            ok = (meta_col_ref[at, 0:1] == meta_row_ref[0:1, :n_keys]) & (meta_row_ref[1:2, :n_keys] <= meta_col_ref[at, 1:2])
            bias_ref[at, :n_keys] = jnp.where(ok, 0.0, -1e30).astype(jnp.float32)

    lo = 0
    for k_part, v_part in zip(k_parts, v_parts):
        hi = lo + k_part.shape[0]
        k_ref[lo:hi, :] = k_part[...]
        v_ref[lo:hi, :] = v_part[...]
        lo = hi
    low = lax.broadcasted_iota(jnp.int32, (Q_TILE, lanes), 1) < head_dim

    def scores(t):
        q = q_ref[t * Q_TILE:(t + 1) * Q_TILE, :]
        zero = jnp.zeros((), q.dtype)
        both = jnp.concatenate([jnp.where(low, q, zero), jnp.where(low, zero, q)], axis=0)
        return lax.dot_general(both, k_ref[:before + (t + 1) * Q_TILE, :], (((1,), (1,)), ((), ())), preferred_element_type=jnp.float32)

    def outputs(t, s):
        at = slice(t * Q_TILE, (t + 1) * Q_TILE)
        n_keys = before + (t + 1) * Q_TILE
        s = s.reshape(2, Q_TILE, n_keys) + bias_ref[at, :n_keys][None]
        e = jnp.exp(s - jnp.max(s, axis=2, keepdims=True))
        total = jnp.sum(e, axis=2, keepdims=True)
        o = jnp.dot(e.astype(jnp.bfloat16).reshape(2 * Q_TILE, n_keys), v_ref[:n_keys, :], preferred_element_type=jnp.float32)
        o = o.reshape(2, Q_TILE, lanes) / total
        o_ref[at, :] = jnp.where(low, o[0], o[1]).astype(o_ref.dtype)

    ahead = scores(0)
    for t in range(n_tiles):
        s = ahead
        if t + 1 < n_tiles:
            ahead = scores(t + 1)
        outputs(t, s)


def attention(q, k_parts, v_parts, doc_ids, positions, head_dim):
    rows, width = q.shape
    n_parts = len(k_parts)
    n_keys = sum(k.shape[0] for k in k_parts)
    lanes = 2 * head_dim
    meta = jnp.stack([doc_ids, positions])[:, :n_keys]
    meta_t = meta[:, n_keys - rows:].T
    head_spec = lambda a: pl.BlockSpec((a.shape[0], lanes), lambda n: (0, n))
    whole = lambda a: pl.BlockSpec(a.shape, lambda n: (0, 0))
    pairs = n_keys * n_keys // 2 - (n_keys - rows) * (n_keys - rows) // 2
    return pl.pallas_call(
        functools.partial(attn_kernel, head_dim, n_parts),
        out_shape=jax.ShapeDtypeStruct((rows, width), jnp.bfloat16),
        grid=(width // lanes,),
        in_specs=[head_spec(a) for a in (q, *k_parts, *v_parts)] + [whole(meta), whole(meta_t)],
        out_specs=head_spec(q),
        scratch_shapes=[pltpu.VMEM((rows, n_keys), jnp.float32), pltpu.VMEM((n_keys, lanes), q.dtype), pltpu.VMEM((n_keys, lanes), q.dtype)],
        compiler_params=pltpu.CompilerParams(vmem_limit_bytes=56 * 1024 * 1024),
        cost_estimate=pl.CostEstimate(flops=16 * pairs * width, bytes_accessed=8 * rows * width, transcendentals=pairs * width // head_dim),
        name="attention",
    )(q, *k_parts, *v_parts, meta, meta_t)


def attn_layer(parts, doc_ids, positions, g_attn, w_q, w_k, w_v, w_o):
    n_heads, head_dim = w_q.shape[1:]
    w_out = w_o.reshape(n_heads * head_dim, -1)
    cos_t, sin_t = rope_tables(positions, head_dim)
    k_parts, v_parts, z_parts = [], [], []
    lo = 0
    for blocks, dest_idx in parts:
        hi = lo + dest_idx.shape[0]
        rows, q, k, v = qkv_proj(blocks, dest_idx, g_attn, w_q, w_k, w_v, cos_t[lo:hi], sin_t[lo:hi])
        k_parts.append(k)
        v_parts.append(v)
        heads = attention(q, k_parts, v_parts, doc_ids, positions, head_dim)
        attn_out = jnp.dot(heads, w_out, preferred_element_type=jnp.float32).astype(jnp.bfloat16)
        z_parts.append((rows.astype(jnp.float32) + attn_out.astype(jnp.float32)).astype(jnp.bfloat16))
        lo = hi
    return z_parts


def relay_tables(group):
    def at(dev, chips_on, flip):
        return (dev // 2 + chips_on) % (group // 2) * 2 + (dev % 2 ^ int(flip))

    relay_of = np.array([[at(i, o, f) for o, f in RELAYS] for i in range(group)])
    source_of = np.array([[at(k, -o, f) for o, f in RELAYS] for k in range(group)])
    return relay_of, source_of


def ceil_div(a, b):
    return -((-a) // b)


def sum_before(x, axis):
    n = x.shape[axis]
    x = jnp.moveaxis(x, axis, -1)
    before = np.arange(n)[:, None] < np.arange(n)[None, :]
    return jnp.moveaxis(jnp.sum(jnp.where(before, x[..., :, None], 0), axis=-2), -1, axis)


def pick(table, index, n):
    return jnp.sum(jnp.where(index[:, None] == jnp.arange(n)[None, :], table[None, :], 0), axis=1)


def run_tables(off_ij, len_ij, n_classes):
    res = np.arange(n_classes)
    first = ceil_div(off_ij[:, None, :] - res[None, :, None], n_classes)
    count = ceil_div((off_ij + len_ij)[:, None, :] - res[None, :, None], n_classes) - first
    return first, count


def out_indices(me, len_ij, lo, n_rows, cap1, cap2, relay_of, source_of):
    group, n_relay = relay_of.shape
    off_all = sum_before(len_ij, 1)
    roff_all = sum_before(len_ij, 0)
    roff_ij = jnp.clip(roff_all, lo, lo + n_rows)
    off_ij = off_all + roff_ij - roff_all
    len_ij = jnp.clip(roff_all + len_ij, lo, lo + n_rows) - roff_ij
    off_ij = jnp.where(len_ij > 0, off_ij, 0)
    first, count = run_tables(off_ij, len_ij, n_relay)
    res = np.arange(n_relay)
    first_k = first[source_of, res]
    count_k = count[source_of, res]
    base_k = sum_before(count_k, 1)

    def mine(t, axis=0):
        return lax.dynamic_index_in_dim(t, me, axis, keepdims=False)

    base_me, count_me, first_me = mine(base_k), mine(count_k), mine(first_k)
    q = jnp.arange(cap2)
    in_m = (q >= base_me[:, :, None]) & (q < (base_me + count_me)[:, :, None])
    src = np.arange(n_relay)[:, None, None] * cap1 + first_me[:, :, None] + q - base_me[:, :, None]
    relay_idx = jnp.sum(jnp.where(in_m, src, 0), axis=0).reshape(-1)

    len_me, off_me, roff_me = mine(len_ij, 1), mine(off_ij, 1), mine(roff_ij, 1)
    base_to_me, first_to_me = mine(base_k, 2), mine(first, 2)
    place = np.zeros((group, n_relay), np.int32)
    place[source_of, res] = np.arange(group)[:, None] * n_relay + res
    table = relay_of * cap2 + base_to_me.reshape(-1)[place] - first_to_me
    u = lo + jnp.arange(n_rows)
    in_i = (u[:, None] >= roff_me[None, :]) & (u[:, None] < (roff_me + len_me)[None, :])
    r_of_u = jnp.sum(jnp.where(in_i, off_me[None, :] + u[:, None] - roff_me[None, :], 0), axis=1)
    i_of_u = jnp.sum(jnp.where(in_i, np.arange(group)[None, :], 0), axis=1)
    dest_idx = pick(table.reshape(-1), i_of_u * n_relay + lax.rem(r_of_u, n_relay), group * n_relay) + r_of_u // n_relay
    return relay_idx, dest_idx


def back_indices(me, len_ij, tok_perm, n_rows, cap1, cap2, source_of, n_chunks):
    group, n_relay = source_of.shape
    n_classes = n_relay * n_chunks
    off_ij = sum_before(len_ij, 1)
    roff_ij = sum_before(len_ij, 0)
    first, count = run_tables(off_ij, len_ij, n_classes)
    cls = (np.arange(n_chunks)[:, None] * n_relay + np.arange(n_relay)[None, :])
    first_k = first[source_of[:, None, :], cls[None]]
    count_k = count[source_of[:, None, :], cls[None]]
    base_k = sum_before(count_k, 2)

    def mine(t, axis=0):
        return lax.dynamic_index_in_dim(t, me, axis, keepdims=False)

    cnt = mine(count_k, 3).transpose(1, 0, 2).reshape(n_chunks, -1)
    fst = mine(first_k, 3).transpose(1, 0, 2).reshape(n_chunks, -1)
    start = sum_before(cnt, 1)
    shift = jnp.broadcast_to(cls[:, None, :] + mine(roff_ij - off_ij, 1)[source_of][None], (n_chunks, group, n_relay)).reshape(n_chunks, -1)
    p = jnp.arange(n_rows)
    in_run = (p >= start[:, :, None]) & (p < (start + cnt)[:, :, None])
    u_of_p = (fst[:, :, None] + p - start[:, :, None]) * n_classes + shift[:, :, None]
    chunk_idx = jnp.sum(jnp.where(in_run, u_of_p + 1, 0), axis=1).reshape(-1) - 1

    n_k = jnp.sum(cnt.reshape(n_chunks, group, n_relay), axis=2)
    start_k = sum_before(n_k, 1)
    q = jnp.arange(cap2)
    far_idx = jnp.where(q < n_k[:, :, None], start_k[:, :, None] + q, -1).reshape(-1)

    base_me, count_me, first_me = mine(base_k), mine(count_k), mine(first_k)
    slot = jnp.arange(cap1)
    in_j = (slot >= first_me[..., None]) & (slot < (first_me + count_me)[..., None])
    back = np.arange(group)[:, None] * cap2 + base_me[..., None] + slot - first_me[..., None]
    near_idx = jnp.sum(jnp.where(in_j, back + 1, 0), axis=2).reshape(-1) - 1

    inv_perm = jnp.argsort(tok_perm)
    group_no = inv_perm // n_relay
    final_idx = (lax.rem(group_no, n_chunks) * n_relay + lax.rem(inv_perm, n_relay)) * cap1 + group_no // n_chunks
    return chunk_idx, far_idx, near_idx, final_idx


N_TILE = 512
FAR_PER = 4
RELAYS = ((0, False), (0, True), (1, False), (1, True), (-1, False), (-1, True))
NEAR_ORDER = (2, 4, 3, 5, 1, 0)
FAR_ORDER = ((2, False), (1, False), (-1, False), (2, True), (1, True), (-1, True), (0, True), (0, False))


def peer(me, group, chips_on, flip):
    n_chips = group // 2
    chip = lax.rem(me // 2 + chips_on + n_chips, n_chips)
    core = lax.rem(me, 2)
    if flip:
        core = 1 - core
    return chip * 2 + core


def row_block(n, most):
    return max(d for d in range(16, most + 1, 16) if n % d == 0)


def build_pick(idx_ref, at, pick_ref, n_src):
    block = row_block(at.size, 288)

    @pl.loop(0, at.size // block)
    def _(b):
        off = pl.multiple_of(b * block, 16)
        lane = lax.broadcasted_iota(jnp.int32, (block, n_src), 1)
        hit = idx_ref[pl.ds(pl.multiple_of(at.start + off, 16), block), :] == lane
        pick_ref[pl.ds(off, block), :n_src] = hit.astype(jnp.float32).astype(pick_ref.dtype)


def gather_rows(src_ref, pick_ref, dst_ref, dst_at):
    n_src, width = src_ref.shape

    @pl.loop(0, width // N_TILE)
    def _(n):
        cols = pl.ds(pl.multiple_of(n * N_TILE, N_TILE), N_TILE)
        rows = jnp.dot(pick_ref[:dst_at.size, :n_src], src_ref[:, cols], preferred_element_type=jnp.float32)
        dst_ref[dst_at, cols] = rows.astype(dst_ref.dtype)


def norm_rows(src_ref, gain_ref, dst_ref):
    block = row_block(src_ref.shape[0], 128)
    gain = gain_ref[...].astype(jnp.float32)

    @pl.loop(0, src_ref.shape[0] // block)
    def _(b):
        at = pl.ds(pl.multiple_of(b * block, 16), block)
        rows_f = src_ref[at, :].astype(jnp.float32)
        inv_rms = lax.rsqrt(jnp.mean(rows_f * rows_f, axis=-1, keepdims=True) + NORM_EPS)
        dst_ref[at, :] = (rows_f * inv_rms * gain).astype(dst_ref.dtype)


def hop(src_ref, idx_ref, pick_ref, buf_ref, land_ref, land_local, cap, targets, per, send_sem, recv_sem, load=None):
    copies, ready = [], []
    for t0 in range(0, len(targets), per):
        for n in range(per):
            block = targets[t0 + n][1]
            build_pick(idx_ref, pl.ds(pl.multiple_of(block * cap, 16), cap), pick_ref.at[pl.ds(n * cap, cap), :], src_ref.shape[0])
        if t0 == 0 and load is not None:
            load.wait()
        for copy in ready:
            copy.start()
        ready = []
        dev, _, slot = targets[t0]
        if per == 1 and dev is None and land_local:
            gather_rows(src_ref, pick_ref, land_ref, pl.ds(pl.multiple_of(slot * cap, 16), cap))
            continue
        gather_rows(src_ref, pick_ref, buf_ref, pl.ds(t0 * cap, per * cap))
        for t in range(t0, t0 + per):
            dev, _, slot = targets[t]
            here = buf_ref.at[pl.ds(t * cap, cap), :]
            there = land_ref.at[pl.ds(pl.multiple_of(slot * cap, 16), cap), :]
            if dev is None:
                ready.append(pltpu.make_async_copy(here, there, recv_sem.at[t]))
            else:
                ready.append(pltpu.make_async_remote_copy(
                    src_ref=here, dst_ref=there, send_sem=send_sem.at[t], recv_sem=recv_sem.at[t],
                    device_id={'sp': dev}, device_id_type=pl.DeviceIdType.MESH))
        copies += ready
    return copies, ready


def two_hop_kernel(group, cap_a, cap_b, rows_ref, idx_a_ref, idx_b_ref, idx_c_ref, out_ref, later_ref, src_ref, pick_ref, buf_a_ref, mid_ref, buf_b_ref,
                   load_sem, sem_a_send, sem_a_recv, sem_b_send, sem_b_recv):
    me = lax.axis_index('sp')
    load = pltpu.make_async_copy(rows_ref, src_ref, load_sem)
    load.start()
    barrier = pltpu.get_barrier_semaphore()
    for other in range(1, group):
        pl.semaphore_signal(barrier, inc=1, device_id={'sp': lax.rem(me + other, group)}, device_id_type=pl.DeviceIdType.MESH)
    pl.semaphore_wait(barrier, group - 1)
    near = []
    for block in NEAR_ORDER:
        chips_on, flip = RELAYS[block]
        near.append((None if (chips_on == 0 and not flip) else peer(me, group, chips_on, flip), block, block))
    far = []
    for chips_on, flip in FAR_ORDER:
        dev = peer(me, group, chips_on, flip)
        far.append((None if (chips_on == 0 and not flip) else dev, dev, me))
    copies, _ = hop(src_ref, idx_a_ref, pick_ref, buf_a_ref, mid_ref, True, cap_a, near, 1, sem_a_send, sem_a_recv, load)
    for copy in copies:
        copy.wait()
    copies, ready = hop(mid_ref, idx_b_ref, pick_ref, buf_b_ref, out_ref, False, cap_b, far, FAR_PER, sem_b_send, sem_b_recv)
    n_later = idx_c_ref.shape[0]
    block = row_block(n_later, pick_ref.shape[0])
    for b in range(n_later // block):
        build_pick(idx_c_ref, pl.ds(b * block, block), pick_ref, mid_ref.shape[0])
        if b == 0:
            for copy in ready:
                copy.start()
        gather_rows(mid_ref, pick_ref, buf_a_ref, pl.ds(b * block, block))
    store = pltpu.make_async_copy(buf_a_ref.at[pl.ds(0, n_later), :], later_ref, load_sem)
    store.start()
    store.wait()
    for copy in copies:
        copy.wait()


def two_hop(src, idx_a, idx_b, idx_c, group, collective_id):
    width = src.shape[1]
    n_a, n_b = len(RELAYS), group
    rows_a, rows_b, rows_c = idx_a.shape[0], idx_b.shape[0], idx_c.shape[0]
    vmem = pl.BlockSpec(memory_space=pltpu.VMEM)
    anywhere = pl.BlockSpec(memory_space=pl.ANY)
    return pl.pallas_call(
        functools.partial(two_hop_kernel, group, rows_a // n_a, rows_b // n_b),
        out_shape=[jax.ShapeDtypeStruct((rows_b, width), src.dtype), jax.ShapeDtypeStruct((rows_c, width), src.dtype)],
        in_specs=[anywhere, vmem, vmem, vmem],
        out_specs=[anywhere, anywhere],
        scratch_shapes=[
            pltpu.VMEM(src.shape, src.dtype),
            pltpu.VMEM((max(rows_a // n_a, FAR_PER * rows_b // n_b), max(src.shape[0], rows_a)), src.dtype),
            pltpu.VMEM((max(rows_a, rows_c), width), src.dtype),
            pltpu.VMEM((rows_a, width), src.dtype),
            pltpu.VMEM((rows_b, width), src.dtype),
            pltpu.SemaphoreType.DMA(()),
            pltpu.SemaphoreType.DMA((n_a,)),
            pltpu.SemaphoreType.DMA((n_a,)),
            pltpu.SemaphoreType.DMA((n_b,)),
            pltpu.SemaphoreType.DMA((n_b,)),
        ],
        compiler_params=pltpu.CompilerParams(collective_id=collective_id, has_side_effects=True, vmem_limit_bytes=60 * 1024 * 1024),
        name="two_hop_out",
    )(src, idx_a[:, None], idx_b[:, None], idx_c[:, None])


FF_TILE = 512
BACK_CHUNKS = 3
PART_SHARE = 3


def mlp_back_kernel(group, n_chunks, cap_far, cap_near, z0_ref, z1_ref, gain_ref, chunk_idx_ref, far_idx_ref, near_idx_ref, wg_ref, wu_ref, wd_ref, out_ref,
                    pick_ref, pick2_ref, zo_ref, h2_ref, acc_ref, buf_ref, mid_ref, far_send, far_recv, near_send, near_recv, z_ref, z_sem):
    h = pl.program_id(0)
    f = pl.program_id(1)
    last_f = pl.num_programs(1) - 1
    n_rows = h2_ref.shape[0]
    block = row_block(n_rows, 80)
    width = z_ref.shape[1]
    n_far = group * cap_far
    n_near = len(RELAYS) * cap_near
    me = lax.axis_index('sp')

    def far_copies(c):
        copies = []
        for t, (chips_on, flip) in enumerate(FAR_ORDER):
            if chips_on == 0 and not flip:
                continue
            dev = peer(me, group, chips_on, flip)
            copies.append(pltpu.make_async_remote_copy(
                src_ref=buf_ref.at[pl.ds(pl.multiple_of(dev * cap_far, 16), cap_far), :],
                dst_ref=mid_ref.at[pl.ds(pl.multiple_of(c * n_far + me * cap_far, 16), cap_far), :],
                send_sem=far_send.at[c, t], recv_sem=far_recv.at[c, t],
                device_id={'sp': dev}, device_id_type=pl.DeviceIdType.MESH))
        return copies

    def near_copies(c):
        copies = []
        for t in NEAR_ORDER:
            chips_on, flip = RELAYS[t]
            src = buf_ref.at[pl.ds(t * cap_near, cap_near), :]
            dst = out_ref.at[pl.ds(c * n_near + t * cap_near, cap_near), :]
            if chips_on == 0 and not flip:
                copies.append(pltpu.make_async_copy(src, dst, near_recv.at[c, t]))
            else:
                copies.append(pltpu.make_async_remote_copy(
                    src_ref=src, dst_ref=dst, send_sem=near_send.at[c, t], recv_sem=near_recv.at[c, t],
                    device_id={'sp': peer(me, group, -chips_on, flip)}, device_id_type=pl.DeviceIdType.MESH))
        return copies

    def start_far(c):
        build_pick(far_idx_ref, pl.ds(c * n_far, n_far), pick_ref, n_rows)
        gather_rows(zo_ref.at[pl.ds(c * n_rows, n_rows), :], pick_ref, buf_ref, pl.ds(0, n_far))
        build_pick(near_idx_ref, pl.ds(c * n_near, n_near), pick2_ref, n_far)
        for copy in far_copies(c):
            copy.start()
        own = pl.multiple_of(me * cap_far, 16)
        mid_ref[pl.ds(pl.multiple_of(c * n_far + own, 16), cap_far), :] = buf_ref[pl.ds(own, cap_far), :]

    def start_near(c):
        for copy in far_copies(c):
            copy.wait()
        gather_rows(mid_ref.at[pl.ds(c * n_far, n_far), :], pick2_ref, buf_ref, pl.ds(0, n_near))
        for copy in near_copies(c):
            copy.start()

    def end_near(c):
        for copy in near_copies(c):
            copy.wait()

    @pl.when((h == 0) & (f == 0))
    def _():
        n_first = z0_ref.shape[0]
        loads = [pltpu.make_async_copy(z0_ref, z_ref.at[pl.ds(0, n_first), :], z_sem.at[0]),
                 pltpu.make_async_copy(z1_ref, z_ref.at[pl.ds(n_first, z1_ref.shape[0]), :], z_sem.at[1])]
        for load in loads:
            load.start()
        for load in loads:
            load.wait()
        barrier = pltpu.get_barrier_semaphore()
        for other in range(1, group):
            pl.semaphore_signal(barrier, inc=1, device_id={'sp': lax.rem(me + other, group)}, device_id_type=pl.DeviceIdType.MESH)
        pl.semaphore_wait(barrier, group - 1)

    for c in range(n_chunks):
        zo = zo_ref.at[pl.ds(c * n_rows, n_rows), :]

        @pl.when((h == c) & (f == 0))
        def _():
            build_pick(chunk_idx_ref, pl.ds(c * n_rows, n_rows), pick_ref, z_ref.shape[0])
            gather_rows(z_ref, pick_ref, zo, pl.ds(0, n_rows))
            norm_rows(zo, gain_ref, h2_ref)
            acc_ref[...] = jnp.zeros(acc_ref.shape, jnp.float32)

        if c > 0:
            @pl.when((h == c) & (f == (last_f + 1) // 2))
            def _():
                start_near(c - 1)

    gate = jnp.dot(h2_ref[...], wg_ref[...], preferred_element_type=jnp.float32)
    up = jnp.dot(h2_ref[...], wu_ref[...], preferred_element_type=jnp.float32)
    act = (gate * jax.nn.sigmoid(gate) * up).astype(jnp.bfloat16)
    acc_ref[...] += jnp.dot(act, wd_ref[...], preferred_element_type=jnp.float32)

    for c in range(n_chunks):
        zo = zo_ref.at[pl.ds(c * n_rows, n_rows), :]

        @pl.when((h == c) & (f == last_f))
        def _():
            if c > 0:
                end_near(c - 1)

            @pl.loop(0, n_rows // block)
            def _(b):
                at = pl.ds(pl.multiple_of(b * block, 16), block)
                down = acc_ref[at, :].astype(jnp.bfloat16).astype(jnp.float32)
                zo[at, :] = (zo[at, :].astype(jnp.float32) + down).astype(zo_ref.dtype)

            start_far(c)
            if c == n_chunks - 1:
                start_near(c)
                end_near(c)


def mlp_back(z_parts, gain, chunk_idx, far_idx, near_idx, w_gate, w_up, w_down, group, n_rows, cap_far, cap_near, collective_id):
    z = z_parts[0]
    width = z.shape[1]
    n_src = sum(part.shape[0] for part in z_parts)
    ff = w_gate.shape[1]
    n_chunks = BACK_CHUNKS
    n_far, n_near = group * cap_far, len(RELAYS) * cap_near
    whole = lambda shape: pl.BlockSpec(shape, lambda h, f: (0, 0), pipeline_mode=pl.Buffered(1))
    return pl.pallas_call(
        functools.partial(mlp_back_kernel, group, n_chunks, cap_far, cap_near),
        out_shape=jax.ShapeDtypeStruct((n_chunks * n_near, width), z.dtype),
        grid=(n_chunks, ff // FF_TILE),
        in_specs=[
            pl.BlockSpec(memory_space=pl.ANY), pl.BlockSpec(memory_space=pl.ANY), whole((1, width)), whole((n_chunks * n_rows, 1)), whole((n_chunks * n_far, 1)), whole((n_chunks * n_near, 1)),
            pl.BlockSpec((width, FF_TILE), lambda h, f: (0, f)),
            pl.BlockSpec((width, FF_TILE), lambda h, f: (0, f)),
            pl.BlockSpec((FF_TILE, width), lambda h, f: (f, 0)),
        ],
        out_specs=pl.BlockSpec(memory_space=pl.ANY),
        scratch_shapes=[
            pltpu.VMEM((max(n_rows, n_far), max(n_src, n_rows)), z.dtype),
            pltpu.VMEM((n_near, n_far), z.dtype),
            pltpu.VMEM((n_chunks * n_rows, width), z.dtype),
            pltpu.VMEM((n_rows, width), z.dtype),
            pltpu.VMEM((n_rows, width), jnp.float32),
            pltpu.VMEM((max(n_far, n_near), width), z.dtype),
            pltpu.VMEM((n_chunks * n_far, width), z.dtype),
            pltpu.SemaphoreType.DMA((n_chunks, group)),
            pltpu.SemaphoreType.DMA((n_chunks, group)),
            pltpu.SemaphoreType.DMA((n_chunks, len(RELAYS))),
            pltpu.SemaphoreType.DMA((n_chunks, len(RELAYS))),
            pltpu.VMEM((n_src, width), z.dtype),
            pltpu.SemaphoreType.DMA((2,)),
        ],
        compiler_params=pltpu.CompilerParams(collective_id=collective_id, has_side_effects=True, vmem_limit_bytes=63 * 1024 * 1024,
                                             dimension_semantics=("arbitrary", "arbitrary")),
        name="mlp_back",
    )(*z_parts, gain.reshape(1, width), chunk_idx[:, None], far_idx[:, None], near_idx[:, None], w_gate, w_up, w_down)


def solution(mesh):
    row_spec = P(('dp', 'sp'), None)
    vec_spec = P(('dp', 'sp'))
    rep_spec = P()

    def per_device(hidden, tok_perm, send_off, send_len, recv_off, recv_len, recv_doc, recv_pos, g_attn, w_q, w_k, w_v, w_o, g_mlp, w_gate, w_up, w_down):
        n_tok, model_dim = hidden.shape
        n_cap = recv_doc.shape[0]
        group = send_off.shape[0]
        relay_of, source_of = relay_tables(group)
        n_relay = relay_of.shape[1]
        round_up = lambda n, unit: -(-n // unit) * unit
        cap1 = round_up(-(-n_tok // n_relay), 16)
        n_first = n_cap // PART_SHARE
        n_parts = (n_first, n_cap - n_first)
        cap2 = [round_up((n + n_relay * (n_relay - 1)) // n_relay, 16) for n in n_parts]
        n_classes = n_relay * BACK_CHUNKS
        cap1_back = round_up(-(-n_tok // n_classes), 16)
        cap2_back = round_up((n_cap + n_relay * (n_classes - 1)) // n_classes, 16)
        n_rows = round_up(-(-(n_cap + group * n_relay * (BACK_CHUNKS - 1)) // BACK_CHUNKS), 16)
        me = lax.axis_index('sp')
        len_ij = lax.all_gather(send_len, 'sp')
        send_idx = jnp.pad(tok_perm, (0, cap1 * n_relay - n_tok)).reshape(cap1, n_relay).T.reshape(-1)
        relay_0, dest_0 = out_indices(me, len_ij, 0, n_parts[0], cap1, cap2[0], relay_of, source_of)
        relay_1, dest_1 = out_indices(me, len_ij, n_first, n_parts[1], cap1, cap2[1], relay_of, source_of)
        chunk_idx, far_idx, near_idx, final_idx = back_indices(me, len_ij, tok_perm, n_rows, cap1_back, cap2_back, source_of, BACK_CHUNKS)

        def take(rows, index):
            return rows.at[index].get(mode='promise_in_bounds')

        blocks_0, later = two_hop(hidden, send_idx, relay_0, relay_1, group, 0)
        blocks_1 = lax.all_to_all(later.reshape(group, cap2[1], model_dim), 'sp', 0, 0, tiled=True).reshape(group * cap2[1], model_dim)
        z_parts = attn_layer([(blocks_0, dest_0), (blocks_1, dest_1)], recv_doc, recv_pos, g_attn, w_q, w_k, w_v, w_o)
        src_back = mlp_back(z_parts, g_mlp, chunk_idx, far_idx, near_idx, w_gate, w_up, w_down, group, n_rows, cap2_back, cap1_back, 1)
        return take(src_back, final_idx)

    return jax.shard_map(per_device, mesh=mesh, in_specs=(row_spec,) + (vec_spec,) * 7 + (rep_spec,) * 9, out_specs=row_spec, check_vma=False)
```

```python
import functools

import jax
import jax.numpy as jnp
import numpy as np
from jax import lax
from jax.experimental import pallas as pl
from jax.experimental.pallas import tpu as pltpu
from jax.sharding import PartitionSpec as P

ROPE_BASE = 500000.0
NORM_EPS = 1e-5
Q_TILE = 256
QKV_TILE = 256


def rope_tables(positions, head_dim):
    half = head_dim // 2
    inv_freq = jnp.power(jnp.float32(ROPE_BASE), -2.0 * jnp.arange(half, dtype=jnp.float32) / head_dim)
    angles = positions.astype(jnp.float32)[:, None] * inv_freq[None, :]
    cos_t = jnp.cos(angles)
    sin_t = jnp.sin(angles)
    return jnp.concatenate([cos_t] * 4, axis=1), jnp.concatenate([-sin_t, sin_t] * 2, axis=1)


def qkv_kernel(head_dim, blocks_ref, idx_ref, gain_ref, cos_ref, sin_ref, wq_ref, wk_ref, wv_ref, r_ref, q_ref, k_ref, v_ref, pick_ref, h_ref):
    n = pl.program_id(0)
    n_each = pl.num_programs(0) // 3
    rows = r_ref.shape[0]
    lanes = cos_ref.shape[1]
    half = head_dim // 2

    @pl.when(n == 0)
    def _():
        build_pick(idx_ref, pl.ds(0, rows), pick_ref, blocks_ref.shape[0])
        gather_rows(blocks_ref, pick_ref, r_ref, pl.ds(0, rows))
        norm_rows(r_ref, gain_ref, h_ref)

    for kind, (w_ref, o_ref) in enumerate(((wq_ref, q_ref), (wk_ref, k_ref), (wv_ref, v_ref))):
        @pl.when(n // n_each == kind)
        def _():
            acc = lax.dot_general(h_ref[...], w_ref[...], (((1,), (1,)), ((), ())), preferred_element_type=jnp.float32)
            if kind == 2:
                o_ref[...] = acc.astype(o_ref.dtype)
                return
            first = lax.rem(lax.broadcasted_iota(jnp.int32, (1, lanes), 1), head_dim) < half
            for b in range(o_ref.shape[1] // lanes):
                x = acc[:, b * lanes:(b + 1) * lanes]
                swapped = jnp.where(first, pltpu.roll(x, lanes - half, 1), pltpu.roll(x, half, 1))
                rot = x * cos_ref[...] + swapped * sin_ref[...]
                if kind == 0:
                    rot = rot * (head_dim ** -0.5)
                o_ref[:, b * lanes:(b + 1) * lanes] = rot.astype(o_ref.dtype)


def qkv_proj(blocks, dest_idx, gain, w_q, w_k, w_v, cos_t, sin_t):
    rows = dest_idx.shape[0]
    model_dim = blocks.shape[1]
    n_heads, head_dim = w_q.shape[1:]
    width = n_heads * head_dim
    n_each = width // QKV_TILE
    w_all = [w.transpose(1, 2, 0).reshape(width, model_dim) for w in (w_q, w_k, w_v)]
    once = lambda shape: pl.BlockSpec(shape, lambda n: (0, 0), pipeline_mode=pl.Buffered(1))
    tile = lambda kind: (lambda n: jnp.clip(n - kind * n_each, 0, n_each - 1))
    return pl.pallas_call(
        functools.partial(qkv_kernel, head_dim),
        out_shape=[jax.ShapeDtypeStruct((rows, model_dim), blocks.dtype)] + [jax.ShapeDtypeStruct((rows, width), blocks.dtype)] * 3,
        grid=(3 * n_each,),
        in_specs=[once(blocks.shape), once((rows, 1)), once((1, model_dim)), once(cos_t.shape), once(sin_t.shape)]
        + [pl.BlockSpec((QKV_TILE, model_dim), lambda n, t=tile(kind): (t(n), 0)) for kind in range(3)],
        out_specs=[once((rows, model_dim))] + [pl.BlockSpec((rows, QKV_TILE), lambda n, t=tile(kind): (0, t(n))) for kind in range(3)],
        scratch_shapes=[pltpu.VMEM((rows, blocks.shape[0]), blocks.dtype), pltpu.VMEM((rows, model_dim), blocks.dtype)],
        compiler_params=pltpu.CompilerParams(vmem_limit_bytes=56 * 1024 * 1024, dimension_semantics=("arbitrary",)),
        cost_estimate=pl.CostEstimate(flops=6 * rows * model_dim * width, bytes_accessed=6 * model_dim * width, transcendentals=0),
        name="qkv",
    )(blocks, dest_idx[:, None], gain.reshape(1, model_dim), cos_t, sin_t, *w_all)


def attn_kernel(head_dim, n_parts, q_ref, *refs):
    k_parts, v_parts = refs[:n_parts], refs[n_parts:2 * n_parts]
    meta_row_ref, meta_col_ref, o_ref, bias_ref, k_ref, v_ref = refs[2 * n_parts:]
    rows, lanes = q_ref.shape
    n_tiles = rows // Q_TILE
    before = k_ref.shape[0] - rows

    @pl.when(pl.program_id(0) == 0)
    def _():
        for t in range(n_tiles):
            at = slice(t * Q_TILE, (t + 1) * Q_TILE)
            n_keys = before + (t + 1) * Q_TILE
            ok = (meta_col_ref[at, 0:1] == meta_row_ref[0:1, :n_keys]) & (meta_row_ref[1:2, :n_keys] <= meta_col_ref[at, 1:2])
            bias_ref[at, :n_keys] = jnp.where(ok, 0.0, -1e30).astype(jnp.float32)

    lo = 0
    for k_part, v_part in zip(k_parts, v_parts):
        hi = lo + k_part.shape[0]
        if n_parts > 1:
            k_ref[lo:hi, :] = k_part[...]
            v_ref[lo:hi, :] = v_part[...]
        lo = hi
    if n_parts == 1:
        k_ref, v_ref = k_parts[0], v_parts[0]
    low = lax.broadcasted_iota(jnp.int32, (Q_TILE, lanes), 1) < head_dim

    def scores(t):
        q = q_ref[t * Q_TILE:(t + 1) * Q_TILE, :]
        zero = jnp.zeros((), q.dtype)
        both = jnp.concatenate([jnp.where(low, q, zero), jnp.where(low, zero, q)], axis=0)
        return lax.dot_general(both, k_ref[:before + (t + 1) * Q_TILE, :], (((1,), (1,)), ((), ())), preferred_element_type=jnp.float32)

    def outputs(t, s):
        at = slice(t * Q_TILE, (t + 1) * Q_TILE)
        n_keys = before + (t + 1) * Q_TILE
        s = s.reshape(2, Q_TILE, n_keys) + bias_ref[at, :n_keys][None]
        e = jnp.exp(s - jnp.max(s, axis=2, keepdims=True))
        total = jnp.sum(e, axis=2, keepdims=True)
        o = jnp.dot(e.astype(jnp.bfloat16).reshape(2 * Q_TILE, n_keys), v_ref[:n_keys, :], preferred_element_type=jnp.float32)
        o = o.reshape(2, Q_TILE, lanes) / total
        o_ref[at, :] = jnp.where(low, o[0], o[1]).astype(o_ref.dtype)

    ahead = scores(0)
    for t in range(n_tiles):
        s = ahead
        if t + 1 < n_tiles:
            ahead = scores(t + 1)
        outputs(t, s)


def attention(q, k_parts, v_parts, doc_ids, positions, head_dim):
    rows, width = q.shape
    n_parts = len(k_parts)
    n_keys = sum(k.shape[0] for k in k_parts)
    lanes = 2 * head_dim
    meta = jnp.stack([doc_ids, positions])[:, :n_keys]
    meta_t = meta[:, n_keys - rows:].T
    head_spec = lambda a: pl.BlockSpec((a.shape[0], lanes), lambda n: (0, n))
    whole = lambda a: pl.BlockSpec(a.shape, lambda n: (0, 0))
    pairs = n_keys * n_keys // 2 - (n_keys - rows) * (n_keys - rows) // 2
    return pl.pallas_call(
        functools.partial(attn_kernel, head_dim, n_parts),
        out_shape=jax.ShapeDtypeStruct((rows, width), jnp.bfloat16),
        grid=(width // lanes,),
        in_specs=[head_spec(a) for a in (q, *k_parts, *v_parts)] + [whole(meta), whole(meta_t)],
        out_specs=head_spec(q),
        scratch_shapes=[pltpu.VMEM((rows, n_keys), jnp.float32), pltpu.VMEM((n_keys, lanes), q.dtype), pltpu.VMEM((n_keys, lanes), q.dtype)],
        compiler_params=pltpu.CompilerParams(vmem_limit_bytes=56 * 1024 * 1024),
        cost_estimate=pl.CostEstimate(flops=16 * pairs * width, bytes_accessed=8 * rows * width, transcendentals=pairs * width // head_dim),
        name="attention",
    )(q, *k_parts, *v_parts, meta, meta_t)


def attn_layer(parts, doc_ids, positions, g_attn, w_q, w_k, w_v, w_o):
    n_heads, head_dim = w_q.shape[1:]
    w_out = w_o.reshape(n_heads * head_dim, -1)
    cos_t, sin_t = rope_tables(positions, head_dim)
    k_parts, v_parts, z_parts = [], [], []
    lo = 0
    for blocks, dest_idx in parts:
        hi = lo + dest_idx.shape[0]
        rows, q, k, v = qkv_proj(blocks, dest_idx, g_attn, w_q, w_k, w_v, cos_t[lo:hi], sin_t[lo:hi])
        k_parts.append(k)
        v_parts.append(v)
        heads = attention(q, k_parts, v_parts, doc_ids, positions, head_dim)
        attn_out = jnp.dot(heads, w_out, preferred_element_type=jnp.float32).astype(jnp.bfloat16)
        z_parts.append((rows.astype(jnp.float32) + attn_out.astype(jnp.float32)).astype(jnp.bfloat16))
        lo = hi
    return z_parts


def relay_tables(group):
    def at(dev, chips_on, flip):
        return (dev // 2 + chips_on) % (group // 2) * 2 + (dev % 2 ^ int(flip))

    relay_of = np.array([[at(i, o, f) for o, f in RELAYS] for i in range(group)])
    source_of = np.array([[at(k, -o, f) for o, f in RELAYS] for k in range(group)])
    return relay_of, source_of


def ceil_div(a, b):
    return -((-a) // b)


def sum_before(x, axis):
    n = x.shape[axis]
    x = jnp.moveaxis(x, axis, -1)
    before = np.arange(n)[:, None] < np.arange(n)[None, :]
    return jnp.moveaxis(jnp.sum(jnp.where(before, x[..., :, None], 0), axis=-2), -1, axis)


def by_relay(x, source_of):
    group = source_of.shape[0]
    mask = source_of.T[:, None, :] == np.arange(group)[:, None]
    rows = []
    for k in range(group):
        mask_k = mask[:, :, k].T.reshape((group,) + (1,) * (x.ndim - 3) + (-1, 1))
        rows.append(jnp.sum(jnp.where(mask_k, x, 0), axis=0))
    return jnp.stack(rows)


def pick(table, index, n):
    return jnp.sum(jnp.where(index[:, None] == jnp.arange(n)[None, :], table[None, :], 0), axis=1)


def run_tables(off_ij, len_ij, n_classes):
    res = np.arange(n_classes)
    first = ceil_div(off_ij[:, None, :] - res[None, :, None], n_classes)
    count = ceil_div((off_ij + len_ij)[:, None, :] - res[None, :, None], n_classes) - first
    return first, count


def out_indices(me, len_ij, lo, n_rows, cap1, cap2, relay_of, source_of):
    group, n_relay = relay_of.shape
    off_all = sum_before(len_ij, 1)
    roff_all = sum_before(len_ij, 0)
    roff_ij = jnp.clip(roff_all, lo, lo + n_rows)
    off_ij = off_all + roff_ij - roff_all
    len_ij = jnp.clip(roff_all + len_ij, lo, lo + n_rows) - roff_ij
    off_ij = jnp.where(len_ij > 0, off_ij, 0)
    first, count = run_tables(off_ij, len_ij, n_relay)
    first_k = by_relay(first, source_of)
    count_k = by_relay(count, source_of)
    base_k = sum_before(count_k, 1)

    def mine(t, axis=0):
        return lax.dynamic_index_in_dim(t, me, axis, keepdims=False)

    base_me, count_me, first_me = mine(base_k), mine(count_k), mine(first_k)
    q = jnp.arange(cap2)
    in_m = (q >= base_me[:, :, None]) & (q < (base_me + count_me)[:, :, None])
    src = np.arange(n_relay)[:, None, None] * cap1 + first_me[:, :, None] + q - base_me[:, :, None]
    relay_idx = jnp.sum(jnp.where(in_m, src, 0), axis=0).reshape(-1)

    len_me, off_me, roff_me = mine(len_ij, 1), mine(off_ij, 1), mine(roff_ij, 1)
    base_to_me, first_to_me = mine(base_k, 2), mine(first, 2)
    base_ic = jnp.sum(jnp.where(relay_of[:, :, None] == np.arange(group), base_to_me.T[None], 0), axis=-1)
    table = relay_of * cap2 + base_ic - first_to_me
    u = lo + jnp.arange(n_rows)
    in_i = (u[:, None] >= roff_me[None, :]) & (u[:, None] < (roff_me + len_me)[None, :])
    r_of_u = jnp.sum(jnp.where(in_i, off_me[None, :] + u[:, None] - roff_me[None, :], 0), axis=1)
    i_of_u = jnp.sum(jnp.where(in_i, np.arange(group)[None, :], 0), axis=1)
    dest_idx = pick(table.reshape(-1), i_of_u * n_relay + lax.rem(r_of_u, n_relay), group * n_relay) + r_of_u // n_relay
    return relay_idx, dest_idx


def back_indices(me, len_ij, tok_perm, n_rows, cap1, cap2, source_of, n_chunks):
    group, n_relay = source_of.shape
    n_classes = n_relay * n_chunks
    off_ij = sum_before(len_ij, 1)
    roff_ij = sum_before(len_ij, 0)
    first, count = run_tables(off_ij, len_ij, n_classes)
    cls = (np.arange(n_chunks)[:, None] * n_relay + np.arange(n_relay)[None, :])
    first_k = by_relay(first.reshape(group, n_chunks, n_relay, group), source_of)
    count_k = by_relay(count.reshape(group, n_chunks, n_relay, group), source_of)
    base_k = sum_before(count_k, 2)

    def mine(t, axis=0):
        return lax.dynamic_index_in_dim(t, me, axis, keepdims=False)

    cnt = mine(count_k, 3).transpose(1, 0, 2).reshape(n_chunks, -1)
    fst = mine(first_k, 3).transpose(1, 0, 2).reshape(n_chunks, -1)
    start = sum_before(cnt, 1)
    moved = jnp.sum(jnp.where(source_of[:, :, None] == np.arange(group), mine(roff_ij - off_ij, 1), 0), axis=-1)
    shift = (cls[:, None, :] + moved[None]).reshape(n_chunks, -1)
    p = jnp.arange(n_rows)
    in_run = (p >= start[:, :, None]) & (p < (start + cnt)[:, :, None])
    u_of_p = (fst[:, :, None] + p - start[:, :, None]) * n_classes + shift[:, :, None]
    chunk_idx = jnp.sum(jnp.where(in_run, u_of_p + 1, 0), axis=1).reshape(-1) - 1

    n_k = jnp.sum(cnt.reshape(n_chunks, group, n_relay), axis=2)
    start_k = sum_before(n_k, 1)
    q = jnp.arange(cap2)
    far_idx = jnp.where(q < n_k[:, :, None], start_k[:, :, None] + q, -1).reshape(-1)

    base_me, count_me, first_me = mine(base_k), mine(count_k), mine(first_k)
    slot = jnp.arange(cap1)
    in_j = (slot >= first_me[..., None]) & (slot < (first_me + count_me)[..., None])
    back = np.arange(group)[:, None] * cap2 + base_me[..., None] + slot - first_me[..., None]
    near_idx = jnp.sum(jnp.where(in_j, back + 1, 0), axis=2).reshape(-1) - 1

    inv_perm = jnp.argsort(tok_perm)
    group_no = inv_perm // n_relay
    final_idx = (lax.rem(group_no, n_chunks) * n_relay + lax.rem(inv_perm, n_relay)) * cap1 + group_no // n_chunks
    return chunk_idx, far_idx, near_idx, final_idx


N_TILE = 512
FAR_PER = 2
RELAYS = ((0, False), (0, True), (1, False), (1, True), (-1, False), (-1, True))
NEAR_ORDER = (2, 4, 3, 5, 1, 0)
FAR_ORDER = ((2, False), (1, False), (-1, False), (2, True), (1, True), (-1, True), (0, True), (0, False))


def peer(me, group, chips_on, flip):
    n_chips = group // 2
    chip = lax.rem(me // 2 + chips_on + n_chips, n_chips)
    core = lax.rem(me, 2)
    if flip:
        core = 1 - core
    return chip * 2 + core


def row_block(n, most):
    return max(d for d in range(16, most + 1, 16) if n % d == 0)


def build_pick(idx_ref, at, pick_ref, n_src):
    block = row_block(at.size, 288)

    @pl.loop(0, at.size // block)
    def _(b):
        off = pl.multiple_of(b * block, 16)
        lane = lax.broadcasted_iota(jnp.int32, (block, n_src), 1)
        hit = idx_ref[pl.ds(pl.multiple_of(at.start + off, 16), block), :] == lane
        pick_ref[pl.ds(off, block), :n_src] = hit.astype(jnp.float32).astype(pick_ref.dtype)


def gather_rows(src_ref, pick_ref, dst_ref, dst_at):
    n_src, width = src_ref.shape

    @pl.loop(0, width // N_TILE)
    def _(n):
        cols = pl.ds(pl.multiple_of(n * N_TILE, N_TILE), N_TILE)
        rows = jnp.dot(pick_ref[:dst_at.size, :n_src], src_ref[:, cols], preferred_element_type=jnp.float32)
        dst_ref[dst_at, cols] = rows.astype(dst_ref.dtype)


def norm_rows(src_ref, gain_ref, dst_ref):
    block = row_block(src_ref.shape[0], 128)
    gain = gain_ref[...].astype(jnp.float32)

    @pl.loop(0, src_ref.shape[0] // block)
    def _(b):
        at = pl.ds(pl.multiple_of(b * block, 16), block)
        rows_f = src_ref[at, :].astype(jnp.float32)
        inv_rms = lax.rsqrt(jnp.mean(rows_f * rows_f, axis=-1, keepdims=True) + NORM_EPS)
        dst_ref[at, :] = (rows_f * inv_rms * gain).astype(dst_ref.dtype)


def hop(src_ref, idx_ref, pick_ref, buf_ref, land_ref, land_local, cap, targets, per, send_sem, recv_sem, load=None):
    copies, ready = [], []
    for t0 in range(0, len(targets), per):
        for n in range(per):
            block = targets[t0 + n][1]
            build_pick(idx_ref, pl.ds(pl.multiple_of(block * cap, 16), cap), pick_ref.at[pl.ds(n * cap, cap), :], src_ref.shape[0])
        if t0 == 0 and load is not None:
            load.wait()
        for copy in ready:
            copy.start()
        ready = []
        dev, _, slot = targets[t0]
        if per == 1 and dev is None and land_local:
            gather_rows(src_ref, pick_ref, land_ref, pl.ds(pl.multiple_of(slot * cap, 16), cap))
            continue
        gather_rows(src_ref, pick_ref, buf_ref, pl.ds(t0 * cap, per * cap))
        for t in range(t0, t0 + per):
            dev, _, slot = targets[t]
            here = buf_ref.at[pl.ds(t * cap, cap), :]
            there = land_ref.at[pl.ds(pl.multiple_of(slot * cap, 16), cap), :]
            if dev is None:
                ready.append(pltpu.make_async_copy(here, there, recv_sem.at[t]))
            else:
                ready.append(pltpu.make_async_remote_copy(
                    src_ref=here, dst_ref=there, send_sem=send_sem.at[t], recv_sem=recv_sem.at[t],
                    device_id={'sp': dev}, device_id_type=pl.DeviceIdType.MESH))
        copies += ready
    return copies, ready


def two_hop_kernel(group, cap_a, cap_b, rows_ref, idx_a_ref, idx_b_ref, idx_c_ref, out_ref, later_ref, src_ref, pick_ref, buf_a_ref, mid_ref, buf_b_ref,
                   load_sem, sem_a_send, sem_a_recv, sem_b_send, sem_b_recv):
    me = lax.axis_index('sp')
    load = pltpu.make_async_copy(rows_ref, src_ref, load_sem)
    load.start()
    barrier = pltpu.get_barrier_semaphore()
    for other in range(1, group):
        pl.semaphore_signal(barrier, inc=1, device_id={'sp': lax.rem(me + other, group)}, device_id_type=pl.DeviceIdType.MESH)
    pl.semaphore_wait(barrier, group - 1)
    near = []
    for block in NEAR_ORDER:
        chips_on, flip = RELAYS[block]
        near.append((None if (chips_on == 0 and not flip) else peer(me, group, chips_on, flip), block, block))
    far = []
    for chips_on, flip in FAR_ORDER:
        dev = peer(me, group, chips_on, flip)
        far.append((None if (chips_on == 0 and not flip) else dev, dev, me))
    copies, _ = hop(src_ref, idx_a_ref, pick_ref, buf_a_ref, mid_ref, True, cap_a, near, 1, sem_a_send, sem_a_recv, load)
    for copy in copies:
        copy.wait()
    copies, ready = hop(mid_ref, idx_b_ref, pick_ref, buf_b_ref, out_ref, False, cap_b, far, FAR_PER, sem_b_send, sem_b_recv)
    n_later = idx_c_ref.shape[0]
    block = row_block(n_later, pick_ref.shape[0])
    for b in range(n_later // block):
        build_pick(idx_c_ref, pl.ds(b * block, block), pick_ref, mid_ref.shape[0])
        if b == 0:
            for copy in ready:
                copy.start()
        gather_rows(mid_ref, pick_ref, buf_a_ref, pl.ds(b * block, block))
    store = pltpu.make_async_copy(buf_a_ref.at[pl.ds(0, n_later), :], later_ref, load_sem)
    store.start()
    store.wait()
    for copy in copies:
        copy.wait()


def two_hop(src, idx_a, idx_b, idx_c, group, collective_id):
    width = src.shape[1]
    n_a, n_b = len(RELAYS), group
    rows_a, rows_b, rows_c = idx_a.shape[0], idx_b.shape[0], idx_c.shape[0]
    vmem = pl.BlockSpec(memory_space=pltpu.VMEM)
    anywhere = pl.BlockSpec(memory_space=pl.ANY)
    return pl.pallas_call(
        functools.partial(two_hop_kernel, group, rows_a // n_a, rows_b // n_b),
        out_shape=[jax.ShapeDtypeStruct((rows_b, width), src.dtype), jax.ShapeDtypeStruct((rows_c, width), src.dtype)],
        in_specs=[anywhere, vmem, vmem, vmem],
        out_specs=[anywhere, anywhere],
        scratch_shapes=[
            pltpu.VMEM(src.shape, src.dtype),
            pltpu.VMEM((max(rows_a // n_a, FAR_PER * rows_b // n_b), max(src.shape[0], rows_a)), src.dtype),
            pltpu.VMEM((max(rows_a, rows_c), width), src.dtype),
            pltpu.VMEM((rows_a, width), src.dtype),
            pltpu.VMEM((rows_b, width), src.dtype),
            pltpu.SemaphoreType.DMA(()),
            pltpu.SemaphoreType.DMA((n_a,)),
            pltpu.SemaphoreType.DMA((n_a,)),
            pltpu.SemaphoreType.DMA((n_b,)),
            pltpu.SemaphoreType.DMA((n_b,)),
        ],
        compiler_params=pltpu.CompilerParams(collective_id=collective_id, has_side_effects=True, vmem_limit_bytes=60 * 1024 * 1024),
        name="two_hop_out",
    )(src, idx_a[:, None], idx_b[:, None], idx_c[:, None])


FF_TILE = 512
BACK_CHUNKS = 3
PART_SHARE = 3


def mlp_back_kernel(group, n_chunks, cap_far, cap_near, z0_ref, z1_ref, gain_ref, chunk_idx_ref, far_idx_ref, near_idx_ref, wg_ref, wu_ref, wd_ref, out_ref,
                    pick_ref, pick2_ref, zo_ref, h2_ref, acc_ref, buf_ref, mid_ref, far_send, far_recv, near_send, near_recv, z_ref, z_sem):
    h = pl.program_id(0)
    f = pl.program_id(1)
    last_f = pl.num_programs(1) - 1
    n_rows = h2_ref.shape[0]
    block = row_block(n_rows, 80)
    width = z_ref.shape[1]
    n_far = group * cap_far
    n_near = len(RELAYS) * cap_near
    me = lax.axis_index('sp')

    def far_copies(c):
        copies = []
        for t, (chips_on, flip) in enumerate(FAR_ORDER):
            if chips_on == 0 and not flip:
                continue
            dev = peer(me, group, chips_on, flip)
            copies.append(pltpu.make_async_remote_copy(
                src_ref=buf_ref.at[pl.ds(pl.multiple_of(dev * cap_far, 16), cap_far), :],
                dst_ref=mid_ref.at[pl.ds(pl.multiple_of(c * n_far + me * cap_far, 16), cap_far), :],
                send_sem=far_send.at[c, t], recv_sem=far_recv.at[c, t],
                device_id={'sp': dev}, device_id_type=pl.DeviceIdType.MESH))
        return copies

    def near_copies(c):
        copies = []
        for t in NEAR_ORDER:
            chips_on, flip = RELAYS[t]
            src = buf_ref.at[pl.ds(t * cap_near, cap_near), :]
            dst = out_ref.at[pl.ds(pl.multiple_of(c * n_near + t * cap_near, 16), cap_near), :]
            if chips_on == 0 and not flip:
                copies.append(pltpu.make_async_copy(src, dst, near_recv.at[c, t]))
            else:
                copies.append(pltpu.make_async_remote_copy(
                    src_ref=src, dst_ref=dst, send_sem=near_send.at[c, t], recv_sem=near_recv.at[c, t],
                    device_id={'sp': peer(me, group, -chips_on, flip)}, device_id_type=pl.DeviceIdType.MESH))
        return copies

    def start_far(c):
        build_pick(far_idx_ref, pl.ds(pl.multiple_of(c * n_far, 16), n_far), pick_ref, n_rows)
        gather_rows(zo_ref.at[pl.ds(pl.multiple_of(c * n_rows, 16), n_rows), :], pick_ref, buf_ref, pl.ds(0, n_far))
        build_pick(near_idx_ref, pl.ds(pl.multiple_of(c * n_near, 16), n_near), pick2_ref, n_far)
        for copy in far_copies(c):
            copy.start()
        own = pl.multiple_of(me * cap_far, 16)
        mid_ref[pl.ds(pl.multiple_of(c * n_far + own, 16), cap_far), :] = buf_ref[pl.ds(own, cap_far), :]

    def start_near(c):
        for copy in far_copies(c):
            copy.wait()
        mid = mid_ref.at[pl.ds(pl.multiple_of(c * n_far, 16), n_far), :]
        n_own = 2 * cap_near
        gather_rows(mid, pick2_ref.at[pl.ds(n_own, n_near - n_own), :], buf_ref, pl.ds(n_own, n_near - n_own))
        copies = near_copies(c)
        for copy in copies[:-2]:
            copy.start()
        gather_rows(mid, pick2_ref, buf_ref, pl.ds(0, n_own))
        for copy in copies[-2:]:
            copy.start()

    def end_near(c):
        for copy in near_copies(c):
            copy.wait()

    @pl.when((h == 0) & (f == 0))
    def _():
        n_first = z0_ref.shape[0]
        loads = [pltpu.make_async_copy(z0_ref, z_ref.at[pl.ds(0, n_first), :], z_sem.at[0]),
                 pltpu.make_async_copy(z1_ref, z_ref.at[pl.ds(n_first, z1_ref.shape[0]), :], z_sem.at[1])]
        for load in loads:
            load.start()
        for load in loads:
            load.wait()
        barrier = pltpu.get_barrier_semaphore()
        for other in range(1, group):
            pl.semaphore_signal(barrier, inc=1, device_id={'sp': lax.rem(me + other, group)}, device_id_type=pl.DeviceIdType.MESH)
        pl.semaphore_wait(barrier, group - 1)

    zo = zo_ref.at[pl.ds(pl.multiple_of(h * n_rows, 16), n_rows), :]

    @pl.when(f == 0)
    def _():
        build_pick(chunk_idx_ref, pl.ds(pl.multiple_of(h * n_rows, 16), n_rows), pick_ref, z_ref.shape[0])
        gather_rows(z_ref, pick_ref, zo, pl.ds(0, n_rows))
        norm_rows(zo, gain_ref, h2_ref)
        acc_ref[...] = jnp.zeros(acc_ref.shape, jnp.float32)

    @pl.when((h > 0) & (f == (last_f + 1) // 2))
    def _():
        start_near(h - 1)

    gate = jnp.dot(h2_ref[...], wg_ref[...], preferred_element_type=jnp.float32)
    up = jnp.dot(h2_ref[...], wu_ref[...], preferred_element_type=jnp.float32)
    act = (gate * jax.nn.sigmoid(gate) * up).astype(jnp.bfloat16)
    acc_ref[...] += jnp.dot(act, wd_ref[...], preferred_element_type=jnp.float32)

    @pl.when((h > 0) & (f == last_f))
    def _():
        end_near(h - 1)

    @pl.when(f == last_f)
    def _():
        @pl.loop(0, n_rows // block)
        def _(b):
            at = pl.ds(pl.multiple_of(b * block, 16), block)
            down = acc_ref[at, :].astype(jnp.bfloat16).astype(jnp.float32)
            zo[at, :] = (zo[at, :].astype(jnp.float32) + down).astype(zo_ref.dtype)

        start_far(h)

    @pl.when((h == n_chunks - 1) & (f == last_f))
    def _():
        start_near(h)
        end_near(h)


def mlp_back(z_parts, gain, chunk_idx, far_idx, near_idx, w_gate, w_up, w_down, group, n_rows, cap_far, cap_near, collective_id):
    z = z_parts[0]
    width = z.shape[1]
    n_src = sum(part.shape[0] for part in z_parts)
    ff = w_gate.shape[1]
    n_chunks = BACK_CHUNKS
    n_far, n_near = group * cap_far, len(RELAYS) * cap_near
    whole = lambda shape: pl.BlockSpec(shape, lambda h, f: (0, 0), pipeline_mode=pl.Buffered(1))
    return pl.pallas_call(
        functools.partial(mlp_back_kernel, group, n_chunks, cap_far, cap_near),
        out_shape=jax.ShapeDtypeStruct((n_chunks * n_near, width), z.dtype),
        grid=(n_chunks, ff // FF_TILE),
        in_specs=[
            pl.BlockSpec(memory_space=pl.ANY), pl.BlockSpec(memory_space=pl.ANY), whole((1, width)), whole((n_chunks * n_rows, 1)), whole((n_chunks * n_far, 1)), whole((n_chunks * n_near, 1)),
            pl.BlockSpec((width, FF_TILE), lambda h, f: (0, f)),
            pl.BlockSpec((width, FF_TILE), lambda h, f: (0, f)),
            pl.BlockSpec((FF_TILE, width), lambda h, f: (f, 0)),
        ],
        out_specs=pl.BlockSpec(memory_space=pl.ANY),
        scratch_shapes=[
            pltpu.VMEM((max(n_rows, n_far), max(n_src, n_rows)), z.dtype),
            pltpu.VMEM((n_near, n_far), z.dtype),
            pltpu.VMEM((n_chunks * n_rows, width), z.dtype),
            pltpu.VMEM((n_rows, width), z.dtype),
            pltpu.VMEM((n_rows, width), jnp.float32),
            pltpu.VMEM((max(n_far, n_near), width), z.dtype),
            pltpu.VMEM((n_chunks * n_far, width), z.dtype),
            pltpu.SemaphoreType.DMA((n_chunks, group)),
            pltpu.SemaphoreType.DMA((n_chunks, group)),
            pltpu.SemaphoreType.DMA((n_chunks, len(RELAYS))),
            pltpu.SemaphoreType.DMA((n_chunks, len(RELAYS))),
            pltpu.VMEM((n_src, width), z.dtype),
            pltpu.SemaphoreType.DMA((2,)),
        ],
        compiler_params=pltpu.CompilerParams(collective_id=collective_id, has_side_effects=True, vmem_limit_bytes=63 * 1024 * 1024,
                                             dimension_semantics=("arbitrary", "arbitrary")),
        name="mlp_back",
    )(*z_parts, gain.reshape(1, width), chunk_idx[:, None], far_idx[:, None], near_idx[:, None], w_gate, w_up, w_down)


def solution(mesh):
    row_spec = P(('dp', 'sp'), None)
    vec_spec = P(('dp', 'sp'))
    rep_spec = P()

    def per_device(hidden, tok_perm, send_off, send_len, recv_off, recv_len, recv_doc, recv_pos, g_attn, w_q, w_k, w_v, w_o, g_mlp, w_gate, w_up, w_down):
        n_tok, model_dim = hidden.shape
        n_cap = recv_doc.shape[0]
        group = send_off.shape[0]
        relay_of, source_of = relay_tables(group)
        n_relay = relay_of.shape[1]
        round_up = lambda n, unit: -(-n // unit) * unit
        cap1 = round_up(-(-n_tok // n_relay), 16)
        n_first = n_cap // PART_SHARE
        n_parts = (n_first, n_cap - n_first)
        cap2 = [round_up((n + n_relay * (n_relay - 1)) // n_relay, 16) for n in n_parts]
        n_classes = n_relay * BACK_CHUNKS
        cap1_back = round_up(-(-n_tok // n_classes), 16)
        cap2_back = round_up((n_cap + n_relay * (n_classes - 1)) // n_classes, 16)
        n_rows = round_up(-(-(n_cap + group * n_relay * (BACK_CHUNKS - 1)) // BACK_CHUNKS), 16)
        me = lax.axis_index('sp')
        len_ij = lax.all_gather(send_len, 'sp')
        send_idx = jnp.pad(tok_perm, (0, cap1 * n_relay - n_tok)).reshape(cap1, n_relay).T.reshape(-1)
        relay_0, dest_0 = out_indices(me, len_ij, 0, n_parts[0], cap1, cap2[0], relay_of, source_of)
        relay_1, dest_1 = out_indices(me, len_ij, n_first, n_parts[1], cap1, cap2[1], relay_of, source_of)
        chunk_idx, far_idx, near_idx, final_idx = back_indices(me, len_ij, tok_perm, n_rows, cap1_back, cap2_back, source_of, BACK_CHUNKS)

        def take(rows, index):
            return rows.at[index].get(mode='promise_in_bounds')

        blocks_0, later = two_hop(hidden, send_idx, relay_0, relay_1, group, 0)
        blocks_1 = lax.all_to_all(later.reshape(group, cap2[1], model_dim), 'sp', 0, 0, tiled=True).reshape(group * cap2[1], model_dim)
        z_parts = attn_layer([(blocks_0, dest_0), (blocks_1, dest_1)], recv_doc, recv_pos, g_attn, w_q, w_k, w_v, w_o)
        src_back = mlp_back(z_parts, g_mlp, chunk_idx, far_idx, near_idx, w_gate, w_up, w_down, group, n_rows, cap2_back, cap1_back, 1)
        return take(src_back, final_idx)

    return jax.shard_map(per_device, mesh=mesh, in_specs=(row_spec,) + (vec_spec,) * 7 + (rep_spec,) * 9, out_specs=row_spec, check_vma=False)
```
